8 devices in a mesh: dp: 1 (over z), tp: 2 (over y), sp: 4 (over x, core).
Axes of the slice: x: 2, y: 2, z: 1, core: 2. Of those that a mesh axis runs over, the one named last changes fastest.
Arguments:
- hidden: bfloat16 [256, 7168], P('dp')
- lat_cache: bfloat16 [256, 2048, 512], P('dp', 'sp')
- rope_cache: bfloat16 [256, 2048, 64], P('dp', 'sp')
- positions: int32 [256], P('dp')
- w_dq: bfloat16 [7168, 1536], replicated
- gain_q: bfloat16 [1536], replicated
- w_dkv: bfloat16 [7168, 576], replicated
- gain_kv: bfloat16 [512], replicated
- w_uq: bfloat16 [1536, 128, 192], P(None, 'tp')
- w_uk: bfloat16 [512, 128, 128], P(None, 'tp')
- w_uv: bfloat16 [512, 128, 128], P(None, 'tp')
- w_out: bfloat16 [16384, 7168], P('tp')
Outputs:
- output 1: bfloat16 [256, 7168], P('dp')
- output 2: bfloat16 [256, 2048, 512], P('dp', 'sp')
- output 3: bfloat16 [256, 2048, 64], P('dp', 'sp')
All inputs are finite; a program needn't handle non-finite values.
Results may differ from the reference program's by a relative error of at most 0.0116136.
Values sent between devices are 32-bit elements.
A program may use at most 2 GiB of HBM per device.

```python
import math
import jax
import jax.numpy as jnp
from jax import lax

BATCH = 256
SEQ = 2048
DMODEL = 7168
HEADS = 128
QRANK = 1536
KVRANK = 512
NOPE = 128
ROPE = 64
VHEAD = 128

EPSILON = 1e-6
ROPE_BASE = 50000.0
SCORE_SCALE = (1.0 + 0.1 * math.log(32.0)) ** 2 / math.sqrt(NOPE + ROPE)
LAT_SPREAD = 1.2
ROPE_SPREAD = 1.7


def setup_inputs(seed: int = 0, part: int = 0) -> dict:
    base_key = jax.random.key(seed)
    shared_keys = jax.random.split(base_key, 8)
    part_keys = jax.random.split(jax.random.fold_in(base_key, part), 5)
    hidden = jax.random.normal(part_keys[0], (BATCH, DMODEL), jnp.float32)
    lat_cache = LAT_SPREAD * jax.random.normal(part_keys[1], (BATCH, SEQ, KVRANK), jnp.float32)
    rope_cache = ROPE_SPREAD * jax.random.normal(part_keys[2], (BATCH, SEQ, ROPE), jnp.float32)
    long_pos = jax.random.randint(part_keys[3], (BATCH,), 0, SEQ, jnp.int32)
    short_pos = jax.random.randint(part_keys[4], (BATCH,), 0, 4, jnp.int32)
    positions = jnp.where(jnp.arange(BATCH) % 4 == 1, short_pos, long_pos)
    positions = positions.at[0].set(SEQ - 1).at[1].set(0)
    w_dq = jax.random.normal(shared_keys[0], (DMODEL, QRANK), jnp.float32) * DMODEL ** -0.5
    gain_q = 1.0 + 0.5 * jax.random.normal(shared_keys[1], (QRANK,), jnp.float32)
    w_dkv = jax.random.normal(shared_keys[2], (DMODEL, KVRANK + ROPE), jnp.float32) * DMODEL ** -0.5
    gain_kv = 1.0 + 0.5 * jax.random.normal(shared_keys[3], (KVRANK,), jnp.float32)
    w_uq = jax.random.normal(shared_keys[4], (QRANK, HEADS, NOPE + ROPE), jnp.float32) * QRANK ** -0.5
    w_uk = jax.random.normal(shared_keys[5], (KVRANK, HEADS, NOPE), jnp.float32) * KVRANK ** -0.5
    w_uv = jax.random.normal(shared_keys[6], (KVRANK, HEADS, VHEAD), jnp.float32) * KVRANK ** -0.5
    w_out = jax.random.normal(shared_keys[7], (HEADS * VHEAD, DMODEL), jnp.float32) * (HEADS * VHEAD) ** -0.5
    return {
        'hidden': hidden.astype(jnp.bfloat16),
        'lat_cache': lat_cache.astype(jnp.bfloat16),
        'rope_cache': rope_cache.astype(jnp.bfloat16),
        'positions': positions,
        'w_dq': w_dq.astype(jnp.bfloat16),
        'gain_q': gain_q.astype(jnp.bfloat16),
        'w_dkv': w_dkv.astype(jnp.bfloat16),
        'gain_kv': gain_kv.astype(jnp.bfloat16),
        'w_uq': w_uq.astype(jnp.bfloat16),
        'w_uk': w_uk.astype(jnp.bfloat16),
        'w_uv': w_uv.astype(jnp.bfloat16),
        'w_out': w_out.astype(jnp.bfloat16),
    }


def rms_norm(values, gain):
    vals32 = values.astype(jnp.float32)
    inv_rms = lax.rsqrt(jnp.mean(vals32 * vals32, axis=-1, keepdims=True) + EPSILON)
    return vals32 * inv_rms * gain.astype(jnp.float32)


def rope_angles(positions):
    half_dim = ROPE // 2
    inv_freq = ROPE_BASE ** (-jnp.arange(half_dim).astype(jnp.float32) / half_dim)
    return positions.astype(jnp.float32)[:, None] * inv_freq[None, :]


def rotate_pairs(values, cos_t, sin_t):
    half_dim = values.shape[-1] // 2
    first_half = values[..., :half_dim]
    second_half = values[..., half_dim:]
    return jnp.concatenate([first_half * cos_t - second_half * sin_t, second_half * cos_t + first_half * sin_t], axis=-1)


def attend_one(operands):
    q_abs, q_rope, lat_all, rope_all, position = operands
    lat32 = lat_all.astype(jnp.float32)
    scores = (jnp.einsum('hk,sk->hs', q_abs.astype(jnp.float32), lat32) + jnp.einsum('hr,sr->hs', q_rope.astype(jnp.float32), rope_all.astype(jnp.float32))) * SCORE_SCALE
    key_valid = jnp.arange(SEQ)[None, :] <= position
    scores = jnp.where(key_valid, scores, -jnp.inf)
    probs = jax.nn.softmax(scores, axis=-1)
    return jnp.einsum('hs,sk->hk', probs, lat32).astype(jnp.bfloat16)


def reference(hidden, lat_cache, rope_cache, positions, w_dq, gain_q, w_dkv, gain_kv, w_uq, w_uk, w_uv, w_out):
    angles = rope_angles(positions)
    cos_t = jnp.cos(angles)
    sin_t = jnp.sin(angles)
    h_q = jnp.dot(hidden, w_dq, preferred_element_type=jnp.float32).astype(jnp.bfloat16)
    c_q = rms_norm(h_q, gain_q).astype(jnp.bfloat16)
    q_full = jnp.einsum('br,rhd->bhd', c_q.astype(jnp.float32), w_uq.astype(jnp.float32)).astype(jnp.bfloat16)
    q_nope = q_full[:, :, :NOPE]
    q_rope = rotate_pairs(q_full[:, :, NOPE:].astype(jnp.float32), cos_t[:, None, :], sin_t[:, None, :]).astype(jnp.bfloat16)
    kv_down = jnp.dot(hidden, w_dkv, preferred_element_type=jnp.float32).astype(jnp.bfloat16)
    lat_new = rms_norm(kv_down[:, :KVRANK], gain_kv).astype(jnp.bfloat16)
    rope_new = rotate_pairs(kv_down[:, KVRANK:].astype(jnp.float32), cos_t, sin_t).astype(jnp.bfloat16)
    slot_hit = (jnp.arange(SEQ)[None, :] == positions[:, None])[:, :, None]
    lat_all = jnp.where(slot_hit, lat_new[:, None, :], lat_cache)
    rope_all = jnp.where(slot_hit, rope_new[:, None, :], rope_cache)
    q_abs = jnp.einsum('bhn,khn->bhk', q_nope.astype(jnp.float32), w_uk.astype(jnp.float32)).astype(jnp.bfloat16)
    o_lat = lax.map(attend_one, (q_abs, q_rope, lat_all, rope_all, positions))
    o_heads = jnp.einsum('bhk,khv->bhv', o_lat.astype(jnp.float32), w_uv.astype(jnp.float32)).astype(jnp.bfloat16)
    attn_out = jnp.dot(o_heads.reshape(BATCH, HEADS * VHEAD), w_out, preferred_element_type=jnp.float32)
    return (hidden.astype(jnp.float32) + attn_out).astype(jnp.bfloat16), lat_all, rope_all
```

```python
import functools
import math
import jax
import jax.numpy as jnp
from jax import lax
from jax.experimental import pallas as pl
from jax.experimental.pallas import tpu as pltpu
from jax.sharding import PartitionSpec as P

EPSILON = 1e-6
ROPE_BASE = 50000.0
YARN_MSCALE = 1.0 + 0.1 * math.log(32.0)
MASK_VALUE = -1e30
MESH = pl.DeviceIdType.MESH
GROUP = 8
SETS = 3
VMEM_LIMIT = 66 * 1000 * 1000


def rms_norm(values, gain):
    vals32 = values.astype(jnp.float32)
    inv_rms = lax.rsqrt(jnp.mean(vals32 * vals32, axis=-1, keepdims=True) + EPSILON)
    return vals32 * inv_rms * gain.astype(jnp.float32)


def rope_tables(positions, rope_dim):
    half_dim = rope_dim // 2
    inv_freq = ROPE_BASE ** (-jnp.arange(half_dim).astype(jnp.float32) / half_dim)
    angles = positions.astype(jnp.float32)[:, None] * inv_freq[None, :]
    return jnp.cos(angles), jnp.sin(angles)


def rotate_pairs(values, cos_t, sin_t):
    half_dim = values.shape[-1] // 2
    first_half = values[..., :half_dim]
    second_half = values[..., half_dim:]
    return jnp.concatenate([first_half * cos_t - second_half * sin_t, second_half * cos_t + first_half * sin_t], axis=-1)


def project_inputs(hidden, positions, w_dq, gain_q, w_dkv, gain_kv, w_uq, w_uk):
    kv_rank = w_uk.shape[0]
    nope_dim = w_uk.shape[2]
    cos_t, sin_t = rope_tables(positions, w_uq.shape[2] - nope_dim)
    h_q = jnp.dot(hidden, w_dq, preferred_element_type=jnp.float32).astype(jnp.bfloat16)
    c_q = rms_norm(h_q, gain_q).astype(jnp.bfloat16)
    q_full = jnp.einsum('br,rhd->bhd', c_q, w_uq, preferred_element_type=jnp.float32).astype(jnp.bfloat16)
    q_rope = rotate_pairs(q_full[:, :, nope_dim:].astype(jnp.float32), cos_t[:, None, :], sin_t[:, None, :]).astype(jnp.bfloat16)
    q_abs = jnp.einsum('bhn,khn->bhk', q_full[:, :, :nope_dim], w_uk, preferred_element_type=jnp.float32).astype(jnp.bfloat16)
    kv_down = jnp.dot(hidden, w_dkv, preferred_element_type=jnp.float32).astype(jnp.bfloat16)
    lat_new = rms_norm(kv_down[:, :kv_rank], gain_kv).astype(jnp.bfloat16)
    rope_new = rotate_pairs(kv_down[:, kv_rank:].astype(jnp.float32), cos_t, sin_t).astype(jnp.bfloat16)
    return q_abs, q_rope, lat_new, rope_new


def attend_kernel(score_scale, n_groups, perm, pos, base, qa, qr, lat_new, rope_new, lat_in, rope_in,
                  lat_out, rope_out, u_out, ml_out, lat_buf, rope_buf, u_buf,
                  lat_rd, rope_rd, lat_wr, rope_wr, u_wr):
    g = pl.program_id(0)
    seq = lat_buf.shape[1]
    heads = qa.shape[1]
    start = base[0]

    def reads(group, slot, j):
        req = perm[group * GROUP + j]
        b = slot * GROUP + j
        return (pltpu.make_async_copy(lat_in.at[req], lat_buf.at[b], lat_rd.at[b]),
                pltpu.make_async_copy(rope_in.at[req], rope_buf.at[b], rope_rd.at[b]))

    def writes(group, slot, j):
        req = perm[group * GROUP + j]
        b = slot * GROUP + j
        return (pltpu.make_async_copy(lat_buf.at[b], lat_out.at[req], lat_wr.at[b]),
                pltpu.make_async_copy(rope_buf.at[b], rope_out.at[req], rope_wr.at[b]))

    lanes = u_buf.shape[1]

    def u_write(group, slot):
        return [pltpu.make_async_copy(u_buf.at[slot, q].reshape(heads, GROUP, 128),
                                      u_out.at[:, pl.ds(group * GROUP, GROUP), pl.ds(q * 128, 128)], u_wr.at[slot, q])
                for q in range(lanes)]

    @pl.when(g == 0)
    def _():
        ml_out[0] = jnp.full(ml_out.shape[1:], MASK_VALUE, jnp.float32)
        ml_out[1] = jnp.zeros(ml_out.shape[1:], jnp.float32)
        for j in range(GROUP):
            for c in reads(0, 0, j):
                c.start()

    nxt = lax.rem(g + 1, SETS)

    @pl.when(g >= SETS - 1)
    def _():
        for j in range(GROUP):
            for c in writes(g - (SETS - 1), nxt, j):
                c.wait()

    @pl.when(g + 1 < n_groups)
    def _():
        for j in range(GROUP):
            for c in reads(g + 1, nxt, j):
                c.start()

    cur = lax.rem(g, SETS)
    uslot = lax.rem(g, 2)

    @pl.when(g >= 2)
    def _():
        for c in u_write(g - 2, uslot):
            c.wait()

    for j in range(GROUP):
        for c in reads(g, cur, j):
            c.wait()

    for j in range(GROUP):
        local = pos[g * GROUP + j] - start
        b = cur * GROUP + j

        @pl.when((local >= 0) & (local < seq))
        def _():
            row0 = pl.multiple_of((local // 16) * 16, 16)
            rows = lat_buf[b, pl.ds(row0, 16), :].astype(jnp.float32)
            hit = lax.broadcasted_iota(jnp.int32, rows.shape, 0) == local - row0
            fresh = jnp.broadcast_to(lat_new[j:j + 1, :].astype(jnp.float32), rows.shape)
            lat_buf[b, pl.ds(row0, 16), :] = jnp.where(hit, fresh, rows).astype(lat_buf.dtype)
            col0 = pl.multiple_of((local // 128) * 128, 128)
            cols = rope_buf[b, :, pl.ds(col0, 128)].astype(jnp.float32)
            hit = lax.broadcasted_iota(jnp.int32, cols.shape, 1) == local - col0
            rope_buf[b, :, pl.ds(col0, 128)] = jnp.where(hit, rope_new[j].astype(jnp.float32), cols).astype(rope_buf.dtype)

    live = pos[g * GROUP] >= start

    @pl.when(live)
    def _():
        lane = lax.broadcasted_iota(jnp.int32, (heads, 128), 1)
        half = g * GROUP // 128
        m_all = ml_out[0, half]
        l_all = ml_out[1, half]
        for j in range(GROUP):
            b = cur * GROUP + j
            i = g * GROUP + j
            lat = lat_buf[b]
            s = lax.dot_general(qa[j], lat, (((1,), (1,)), ((), ())), preferred_element_type=jnp.float32)
            s += jnp.dot(qr[j], rope_buf[b], preferred_element_type=jnp.float32)
            s *= score_scale
            valid = lax.broadcasted_iota(jnp.int32, s.shape, 1) <= pos[i] - start
            s = jnp.where(valid, s, MASK_VALUE)
            m = jnp.max(s, axis=1, keepdims=True)
            w = jnp.where(valid, jnp.exp(s - m), 0.0)
            l = jnp.sum(w, axis=1, keepdims=True)
            u = jnp.dot(w.astype(jnp.bfloat16), lat, preferred_element_type=jnp.float32)
            for q in range(lanes):
                u_buf[uslot, q, pl.ds(j, heads, stride=GROUP), :] = u[:, q * 128:(q + 1) * 128]
            here = lane == i - half * 128
            m_all = jnp.where(here, m, m_all)
            l_all = jnp.where(here, l, l_all)
        ml_out[0, half] = m_all
        ml_out[1, half] = l_all

    @pl.when(jnp.logical_not(live))
    def _():
        u_buf[uslot] = jnp.zeros(u_buf.shape[1:], jnp.float32)

    for j in range(GROUP):
        for c in writes(g, cur, j):
            c.start()
    for c in u_write(g, uslot):
        c.start()

    @pl.when(g == n_groups - 1)
    def _():
        for k in range(SETS - 1):
            for j in range(GROUP):
                for c in writes(g - k, lax.rem(g - k, SETS), j):
                    c.wait()
        for k in range(2):
            for c in u_write(g - k, lax.rem(g - k, 2)):
                c.wait()


def attend(perm, pos, base, qa, qr, lat_new, rope_new, lat_cache, rope_t, score_scale):
    rows, heads, rank = qa.shape
    seq = lat_cache.shape[1]
    rope_dim = qr.shape[2]
    n_groups = rows // GROUP
    any_spec = pl.BlockSpec(memory_space=pl.ANY)
    return pl.pallas_call(
        functools.partial(attend_kernel, score_scale, n_groups),
        grid_spec=pltpu.PrefetchScalarGridSpec(
            num_scalar_prefetch=3,
            grid=(n_groups,),
            in_specs=[
                pl.BlockSpec((GROUP, heads, rank), lambda g, *_: (g, 0, 0)),
                pl.BlockSpec((GROUP, heads, rope_dim), lambda g, *_: (g, 0, 0)),
                pl.BlockSpec((GROUP, rank), lambda g, *_: (g, 0)),
                pl.BlockSpec((GROUP, rope_dim, 128), lambda g, *_: (g, 0, 0)),
                any_spec, any_spec,
            ],
            out_specs=[any_spec, any_spec, any_spec,
                       pl.BlockSpec((2, rows // 128, heads, 128), lambda g, *_: (0, 0, 0, 0))],
            scratch_shapes=[
                pltpu.VMEM((SETS * GROUP, seq, rank), jnp.bfloat16),
                pltpu.VMEM((SETS * GROUP, rope_dim, seq), jnp.bfloat16),
                pltpu.VMEM((2, rank // 128, heads * GROUP, 128), jnp.float32),
                pltpu.SemaphoreType.DMA((SETS * GROUP,)),
                pltpu.SemaphoreType.DMA((SETS * GROUP,)),
                pltpu.SemaphoreType.DMA((SETS * GROUP,)),
                pltpu.SemaphoreType.DMA((SETS * GROUP,)),
                pltpu.SemaphoreType.DMA((2, rank // 128)),
            ],
        ),
        out_shape=[
            jax.ShapeDtypeStruct(lat_cache.shape, lat_cache.dtype),
            jax.ShapeDtypeStruct(rope_t.shape, rope_t.dtype),
            jax.ShapeDtypeStruct((heads, rows, rank), jnp.float32),
            jax.ShapeDtypeStruct((2, rows // 128, heads, 128), jnp.float32),
        ],
        compiler_params=pltpu.CompilerParams(dimension_semantics=("arbitrary",), vmem_limit_bytes=48 * 1024 * 1024),
        name="attend",
    )(perm, pos, base, qa, qr, lat_new, rope_new, lat_cache, rope_t)


CH = 4


def combine_kernel(n_cross, u_ref, f_ref, wuv_ref, wout_ref, att_ref,
                   d_buf, own_buf, f_buf, x_buf, o_out, o_in, o_all, w_buf, p_buf, y_buf, wuv_buf,
                   d_ss, d_rs, x_ss, x_rs, o_ss, o_rs, y_ss, y_rs, h_ss, h_rs, c_ss, c_rs, w_ss, w_rs,
                   own_sem, f_sem, wt_sem, loc_sem, wuv_sem):
    hh, rows, rank = d_buf.shape
    half = n_cross // 2
    r_own = rows - half
    vdim = wuv_buf.shape[2]
    n_chunk = hh // CH
    n_blk, _, bcol = p_buf.shape
    tp = lax.axis_index('tp')
    sp = lax.axis_index('sp')
    core = lax.rem(sp, 2)
    x = sp // 2
    mate = x * 2 + (1 - core)
    across = (1 - x) * 2 + core
    to_mate = {'dp': lax.axis_index('dp'), 'tp': tp, 'sp': mate}
    to_x = {'dp': lax.axis_index('dp'), 'tp': tp, 'sp': across}
    to_y = {'dp': lax.axis_index('dp'), 'tp': 1 - tp, 'sp': sp}

    def remote(src, dst, ss, rs, dev):
        return pltpu.make_async_remote_copy(src_ref=src, dst_ref=dst, send_sem=ss, recv_sem=rs,
                                            device_id=dev, device_id_type=MESH)

    barrier = pltpu.get_barrier_semaphore()
    for dev in (to_mate, to_x, to_y):
        pl.semaphore_signal(barrier, inc=1, device_id=dev, device_id_type=MESH)

    def own_load(k):
        hs = pl.ds(k * CH, CH)
        return (pltpu.make_async_copy(u_ref.at[pl.ds(core * hh + k * CH, CH)], own_buf.at[lax.rem(k, 2)], own_sem.at[lax.rem(k, 2)]),
                pltpu.make_async_copy(f_ref.at[:, hs], f_buf.at[lax.rem(k, 2)], f_sem.at[lax.rem(k, 2)]))

    def w_load(j):
        col = pl.multiple_of(core * (n_blk * bcol) + j * bcol, 128)
        return pltpu.make_async_copy(wout_ref.at[:, pl.ds(col, bcol)], w_buf.at[lax.rem(j, 2)], wt_sem.at[lax.rem(j, 2)])

    for k in range(2):
        for c in own_load(k):
            c.start()
    wuv_load = pltpu.make_async_copy(wuv_ref, wuv_buf, wuv_sem)
    pl.semaphore_wait(barrier, 3)

    def d_copy(k):
        return remote(u_ref.at[pl.ds((1 - core) * hh + k * CH, CH)], d_buf.at[pl.ds(k * CH, CH)],
                      d_ss.at[k], d_rs.at[k], to_mate)

    for k in range(n_chunk):
        d_copy(k).start()
    wuv_load.start()
    for j in range(2):
        w_load(j).start()

    give = pl.multiple_of((1 - x) * half, 8)
    keep = pl.multiple_of(x * half, 8)

    def x_copy(k):
        return remote(d_buf.at[pl.ds(k * CH, CH), pl.ds(give, half), :], x_buf.at[pl.ds(k * CH, CH)],
                      x_ss.at[k], x_rs.at[k], to_x)

    def o_copy(k):
        return remote(o_out.at[pl.ds(k * CH, CH)], o_in.at[pl.ds(k * CH, CH)], o_ss.at[k], o_rs.at[k], to_mate)

    rb = 64

    def reduce_chunk(k, _):
        for c in own_load(k):
            c.wait()
        d_copy(k).wait_recv()
        slot = lax.rem(k, 2)

        def scale(t, _):
            a = t // (rows // rb)
            r0 = pl.multiple_of(lax.rem(t, rows // rb) * rb, rb)
            fo = f_buf[slot, 0, a, pl.ds(r0, rb), :]
            fm = f_buf[slot, 1, a, pl.ds(r0, rb), :]
            for q in range(rank // 128):
                cs = pl.ds(q * 128, 128)
                mine = own_buf[slot, a, pl.ds(r0, rb), cs]
                theirs = d_buf[k * CH + a, pl.ds(r0, rb), cs]
                d_buf[k * CH + a, pl.ds(r0, rb), cs] = fo * mine + fm * theirs
            return 0

        lax.fori_loop(0, CH * (rows // rb), scale, 0)
        x_copy(k).start()

        @pl.when(k + 2 < n_chunk)
        def _():
            for c in own_load(k + 2):
                c.start()
        return 0

    lax.fori_loop(0, n_chunk, reduce_chunk, 0)
    wuv_load.wait()

    def project_chunk(k, _):
        x_copy(k).wait_recv()

        def project(a, _):
            h = k * CH + a
            crossing = d_buf[h, pl.ds(keep, half), :] + x_buf[h]
            parts = [crossing]
            if n_cross < rows:
                parts.append(d_buf[h, pl.ds(n_cross, rows - n_cross), :])
            u = (jnp.concatenate(parts, axis=0) if len(parts) > 1 else crossing).astype(jnp.bfloat16)
            o = jnp.dot(u, wuv_buf[h], preferred_element_type=jnp.float32).astype(jnp.bfloat16)
            o_all[:, pl.ds(pl.multiple_of((core * hh + h) * vdim, 128), vdim)] = o
            o_out[h] = o.astype(jnp.float32)
            return 0

        lax.fori_loop(0, CH, project, 0)
        o_copy(k).start()
        return 0

    lax.fori_loop(0, n_chunk, project_chunk, 0)

    def place_chunk(k, _):
        o_copy(k).wait_recv()

        def place(a, _):
            h = k * CH + a
            o_all[:, pl.ds(pl.multiple_of(((1 - core) * hh + h) * vdim, 128), vdim)] = o_in[h].astype(jnp.bfloat16)
            return 0

        lax.fori_loop(0, CH, place, 0)
        return 0

    lax.fori_loop(0, n_chunk, place_chunk, 0)

    def cols(j):
        return pl.ds(pl.multiple_of(core * (n_blk * bcol) + j * bcol, 128), bcol)

    def y_copy(j):
        return remote(p_buf.at[j], y_buf.at[j], y_ss.at[j], y_rs.at[j], to_y)

    def c_copy(j):
        return remote(y_buf.at[j], att_ref.at[x, :, cols(j)], c_ss.at[j], c_rs.at[j], to_mate)

    def h_copy(j):
        return remote(y_buf.at[j], att_ref.at[x, :, cols(j)], h_ss.at[j], h_rs.at[j], to_x)

    def w_copy(j):
        return remote(att_ref.at[1 - x, :, cols(j)], att_ref.at[1 - x, :, cols(j)], w_ss.at[j], w_rs.at[j], to_mate)

    def l_copy(j):
        return pltpu.make_async_copy(y_buf.at[j], att_ref.at[x, :, cols(j)], loc_sem.at[j])

    def total(j):
        y_copy(j).wait_recv()
        y_buf[j] = y_buf[j] + p_buf[j]
        h_copy(j).start()
        c_copy(j).start()
        l_copy(j).start()

    def forward(j):
        h_copy(j).wait_recv()
        w_copy(j).start()

    early = (4, 8, 11)

    def block(j, _):
        w_load(j).wait()
        p_buf[j] = jnp.dot(o_all[...], w_buf[lax.rem(j, 2)], preferred_element_type=jnp.float32)
        y_copy(j).start()

        @pl.when(j + 2 < n_blk)
        def _():
            w_load(j + 2).start()

        for i, at in enumerate(early):
            @pl.when(j == at)
            def _(i=i):
                total(i)
        return 0

    lax.fori_loop(0, n_blk, block, 0)

    def finish(j, _):
        total(j)
        forward(j - len(early))
        return 0

    lax.fori_loop(len(early), n_blk, finish, 0)
    for j in range(n_blk - len(early), n_blk):
        forward(j)

    def drain(k, _):
        d_copy(k).wait_send()
        x_copy(k).wait_send()
        o_copy(k).wait_send()
        return 0

    lax.fori_loop(0, n_chunk, drain, 0)

    def drain_blocks(j, _):
        y_copy(j).wait_send()
        h_copy(j).wait_send()
        c_copy(j).wait()
        w_copy(j).wait()
        l_copy(j).wait()
        return 0

    lax.fori_loop(0, n_blk, drain_blocks, 0)


def combine(n_cross, cid, u, f, wuv, wout):
    heads, rows, rank = u.shape
    hh = heads // 2
    vdim = wuv.shape[2]
    depth, width = wout.shape
    half = n_cross // 2
    r_own = rows - half
    bcol = 256
    n_blk = width // 2 // bcol
    n_chunk = hh // CH
    dma = pltpu.SemaphoreType.DMA
    return pl.pallas_call(
        functools.partial(combine_kernel, n_cross),
        in_specs=[pl.BlockSpec(memory_space=pl.ANY)] * 4,
        out_specs=pl.BlockSpec(memory_space=pl.ANY),
        out_shape=jax.ShapeDtypeStruct((2, r_own, width), jnp.float32),
        scratch_shapes=[
            pltpu.VMEM((hh, rows, rank), jnp.float32),
            pltpu.VMEM((2, CH, rows, rank), jnp.float32),
            pltpu.VMEM((2, 2, CH, rows, 128), jnp.float32),
            pltpu.VMEM((hh, half, rank), jnp.float32),
            pltpu.VMEM((hh, r_own, vdim), jnp.float32),
            pltpu.VMEM((hh, r_own, vdim), jnp.float32),
            pltpu.VMEM((r_own, depth), jnp.bfloat16),
            pltpu.VMEM((2, depth, bcol), jnp.bfloat16),
            pltpu.VMEM((n_blk, r_own, bcol), jnp.float32),
            pltpu.VMEM((n_blk, r_own, bcol), jnp.float32),
            pltpu.VMEM((hh, rank, vdim), jnp.bfloat16),
        ] + [dma((n_chunk,))] * 6 + [dma((n_blk,))] * 8 + [dma((2,))] * 3 + [dma((n_blk,)), dma(())],
        compiler_params=pltpu.CompilerParams(collective_id=cid, has_side_effects=True, vmem_limit_bytes=VMEM_LIMIT),
        name=f"combine{n_cross}",
    )(u, f, wuv, wout)


def solution(mesh):
    row_spec = P('dp', None)
    cache_spec = P('dp', 'sp', None)
    head_spec = P(None, 'tp', None)
    in_specs = (row_spec, cache_spec, cache_spec, P('dp'), P(), P(), P(), P(), head_spec, head_spec, head_spec, P('tp', None))
    out_specs = (row_spec, cache_spec, cache_spec)
    n_sp = mesh.shape['sp']

    def local_step(hidden, lat_cache, rope_cache, positions, w_dq, gain_q, w_dkv, gain_kv, w_uq, w_uk, w_uv, w_out):
        rows = hidden.shape[0]
        seq = lat_cache.shape[1]
        heads = w_uk.shape[1]
        hh = heads // 2
        score_scale = YARN_MSCALE ** 2 / math.sqrt(w_uq.shape[2])
        sp = lax.axis_index('sp')
        core = lax.rem(sp, 2)

        idx = jnp.arange(rows)
        before = (positions[None, :] > positions[:, None]) | ((positions[None, :] == positions[:, None]) & (idx[None, :] < idx[:, None]))
        rank = jnp.sum(before.astype(jnp.int32), axis=1)
        sel = rank[None, :] == idx[:, None]
        perm = jnp.sum(jnp.where(sel, idx[None, :], 0), axis=1).astype(jnp.int32)
        pos_s = jnp.sum(jnp.where(sel, positions[None, :], 0), axis=1).astype(jnp.int32)
        sel16 = sel.astype(jnp.bfloat16)
        hidden_s = jnp.dot(sel16, hidden, preferred_element_type=jnp.float32).astype(jnp.bfloat16)

        q_abs, q_rope, lat_new, rope_new = project_inputs(hidden_s, pos_s, w_dq, gain_q, w_dkv, gain_kv, w_uq, w_uk)
        rope_wide = jnp.broadcast_to(rope_new[:, :, None], rope_new.shape + (128,))
        base = (sp * seq).astype(jnp.int32).reshape(1)
        lat_out, rope_out, u_part, ml = attend(perm, pos_s, base, q_abs, q_rope, lat_new, rope_wide,
                                               lat_cache, rope_cache.transpose(0, 2, 1), score_scale)

        ml = ml.transpose(0, 2, 1, 3).reshape(2, heads, rows)
        ml_all = lax.all_gather(ml, 'sp')
        m_all, l_all = ml_all[:, 0], ml_all[:, 1]
        e_all = jnp.exp(m_all - jnp.max(m_all, axis=0, keepdims=True))
        f_all = e_all / jnp.sum(e_all * l_all, axis=0, keepdims=True)
        mate = sp + 1 - 2 * core
        f_half = lax.dynamic_slice_in_dim(f_all, core * hh, hh, axis=1)
        f_pair = jnp.stack([lax.dynamic_index_in_dim(f_half, sp, 0, False), lax.dynamic_index_in_dim(f_half, mate, 0, False)])
        f_wide = jnp.broadcast_to(f_pair[..., None], f_pair.shape + (128,))
        wuv_half = lax.dynamic_slice_in_dim(w_uv, core * hh, hh, axis=1).transpose(1, 0, 2)

        n_over = jnp.sum((positions >= (n_sp // 2) * seq).astype(jnp.int32))
        sizes = sorted({min(rows, max(16, s * rows // 256)) for s in (64, 96, 112, 160, 256)})
        which = sum((n_over > s).astype(jnp.int32) for s in sizes[:-1])

        def branch(n_cross, cid):
            def run(u, f, wuv, wout, rank, hidden, sel16):
                att = combine(n_cross, cid, u, f, wuv, wout)
                half = n_cross // 2
                att = jnp.concatenate([att[0, :half], att[1, :half], att[0, half:]], axis=0)
                hid = jnp.dot(sel16, hidden, preferred_element_type=jnp.float32)
                return (hid + att).astype(jnp.bfloat16)
            return run

        out_s = lax.switch(which, [branch(s, i) for i, s in enumerate(sizes)], u_part, f_wide, wuv_half, w_out, rank, hidden, sel16)
        out = lax.dot_general(sel16, out_s, (((0,), (0,)), ((), ())), preferred_element_type=jnp.float32).astype(jnp.bfloat16)
        return out, lat_out, rope_out.transpose(0, 2, 1)

    return jax.shard_map(local_step, mesh=mesh, in_specs=in_specs, out_specs=out_specs, check_vma=False)
```

```python
import functools
import math
import jax
import jax.numpy as jnp
from jax import lax
from jax.experimental import pallas as pl
from jax.experimental.pallas import tpu as pltpu
from jax.sharding import PartitionSpec as P

EPSILON = 1e-6
ROPE_BASE = 50000.0
YARN_MSCALE = 1.0 + 0.1 * math.log(32.0)
MASK_VALUE = -1e30
MESH = pl.DeviceIdType.MESH
GROUP = 8
SETS = 4
AHEAD = 2
VMEM_LIMIT = 66 * 1000 * 1000
SIZES = (96, 112, 160, 256)


def rms_norm(values, gain):
    vals32 = values.astype(jnp.float32)
    inv_rms = lax.rsqrt(jnp.mean(vals32 * vals32, axis=-1, keepdims=True) + EPSILON)
    return vals32 * inv_rms * gain.astype(jnp.float32)


def rope_tables(positions, rope_dim):
    half_dim = rope_dim // 2
    inv_freq = ROPE_BASE ** (-jnp.arange(half_dim).astype(jnp.float32) / half_dim)
    angles = positions.astype(jnp.float32)[:, None] * inv_freq[None, :]
    return jnp.cos(angles), jnp.sin(angles)


def rotate_pairs(values, cos_t, sin_t):
    half_dim = values.shape[-1] // 2
    first_half = values[..., :half_dim]
    second_half = values[..., half_dim:]
    return jnp.concatenate([first_half * cos_t - second_half * sin_t, second_half * cos_t + first_half * sin_t], axis=-1)


def query_kernel(cq, cos_w, sin_w, wq, wk, q_out, k_buf, a_buf, r_buf):
    rows = cq.shape[0]
    heads, _, _ = wq.shape
    rank = wk.shape[0]
    nope = wk.shape[2]
    half = (wq.shape[1] - nope) // 2
    nt = (((1,), (1,)), ((), ()))
    k_buf[...] = wk[...].astype(jnp.float32).reshape(rank * heads, nope)
    for h in range(heads):
        q = lax.dot_general(cq[...], wq[h], nt, preferred_element_type=jnp.float32).astype(jnp.bfloat16)
        r = q[:, nope:].astype(jnp.float32)
        r = r * cos_w[...] + jnp.concatenate([r[:, half:], r[:, :half]], axis=1) * sin_w[...]
        r_buf[pl.ds(h, rows, stride=heads), :] = jnp.concatenate([r, jnp.zeros((rows, 128 - 2 * half), jnp.float32)], axis=1)
        wk_h = k_buf[pl.ds(h, rank, stride=heads), :].astype(jnp.bfloat16)
        qa = lax.dot_general(q[:, :nope], wk_h, nt, preferred_element_type=jnp.float32)
        for c in range(rank // 128):
            a_buf[c, pl.ds(h, rows, stride=heads), :] = qa[:, c * 128:(c + 1) * 128]
    for c in range(rank // 128):
        q_out[:, :, c * 128:(c + 1) * 128] = a_buf[c].reshape(rows, heads, 128).astype(q_out.dtype)
    q_out[:, :, rank:] = r_buf[...].reshape(rows, heads, 128).astype(q_out.dtype)


def queries(cq, cos_w, sin_w, w_uq, w_uk):
    rows, qrank = cq.shape
    wq = w_uq.transpose(1, 2, 0)
    heads, width, _ = wq.shape
    rank, _, nope = w_uk.shape
    hb = 8
    rope_dim = width - nope
    return pl.pallas_call(
        query_kernel,
        grid=(heads // hb,),
        in_specs=[
            pl.BlockSpec((rows, qrank), lambda i: (0, 0)),
            pl.BlockSpec((rows, rope_dim), lambda i: (0, 0)),
            pl.BlockSpec((rows, rope_dim), lambda i: (0, 0)),
            pl.BlockSpec((hb, width, qrank), lambda i: (i, 0, 0)),
            pl.BlockSpec((rank, hb, nope), lambda i: (0, i, 0)),
        ],
        out_specs=pl.BlockSpec((rows, hb, rank + 128), lambda i: (0, i, 0)),
        out_shape=jax.ShapeDtypeStruct((rows, heads, rank + 128), jnp.bfloat16),
        scratch_shapes=[
            pltpu.VMEM((rank * hb, nope), jnp.float32),
            pltpu.VMEM((rank // 128, rows * hb, 128), jnp.float32),
            pltpu.VMEM((rows * hb, 128), jnp.float32),
        ],
        compiler_params=pltpu.CompilerParams(dimension_semantics=("arbitrary",), vmem_limit_bytes=48 * 1024 * 1024),
        cost_estimate=pl.CostEstimate(flops=2 * rows * heads * (width * qrank + nope * rank), bytes_accessed=70_000_000, transcendentals=0),
        name="queries",
    )(cq, cos_w, sin_w, wq, w_uk)


def project_inputs(hidden, positions, w_dq, gain_q, w_dkv, gain_kv, w_uq, w_uk):
    kv_rank = w_uk.shape[0]
    nope_dim = w_uk.shape[2]
    cos_t, sin_t = rope_tables(positions, w_uq.shape[2] - nope_dim)
    h_q = jnp.dot(hidden, w_dq, preferred_element_type=jnp.float32).astype(jnp.bfloat16)
    c_q = rms_norm(h_q, gain_q).astype(jnp.bfloat16)
    query = queries(c_q, jnp.concatenate([cos_t, cos_t], axis=1), jnp.concatenate([-sin_t, sin_t], axis=1), w_uq, w_uk)
    kv_down = jnp.dot(hidden, w_dkv, preferred_element_type=jnp.float32).astype(jnp.bfloat16)
    lat_new = rms_norm(kv_down[:, :kv_rank], gain_kv).astype(jnp.bfloat16)
    rope_new = rotate_pairs(kv_down[:, kv_rank:].astype(jnp.float32), cos_t, sin_t).astype(jnp.bfloat16)
    return query, lat_new, rope_new


def attend_kernel(score_scale, n_groups, first, n_alias, perm, pos, base, query, lat_new, rope_new, lat_in, rope_in, *rest):
    (lat_out, rope_out, u_out, ml_out, lat_buf, rope_buf, u_buf,
     lat_rd, rope_rd, lat_wr, rope_wr, u_wr) = rest[n_alias:]
    g = pl.program_id(0)
    seq = lat_buf.shape[1]
    rank = lat_buf.shape[2]
    rope_dim = rope_buf.shape[1]
    heads = query.shape[1]
    start = base[0]
    rope_cols = rope_new[...].astype(jnp.float32).T

    def reads(group, slot, j):
        req = perm[first + group * GROUP + j]
        b = slot * GROUP + j
        return (pltpu.make_async_copy(lat_in.at[req], lat_buf.at[b], lat_rd.at[b]),
                pltpu.make_async_copy(rope_in.at[req], rope_buf.at[b], rope_rd.at[b]))

    def writes(group, slot, j):
        req = perm[first + group * GROUP + j]
        b = slot * GROUP + j
        return (pltpu.make_async_copy(lat_buf.at[b], lat_out.at[req], lat_wr.at[b]),
                pltpu.make_async_copy(rope_buf.at[b], rope_out.at[req], rope_wr.at[b]))

    lanes = u_buf.shape[1]

    def u_write(group, slot):
        return [pltpu.make_async_copy(u_buf.at[slot, q].reshape(heads, GROUP, 128),
                                      u_out.at[:, pl.ds(group * GROUP, GROUP), pl.ds(q * 128, 128)], u_wr.at[slot, q])
                for q in range(lanes)]

    @pl.when(g == 0)
    def _():
        ml_out[0] = jnp.full(ml_out.shape[1:], MASK_VALUE, jnp.float32)
        ml_out[1] = jnp.zeros(ml_out.shape[1:], jnp.float32)
        for a in range(AHEAD):
            for j in range(GROUP):
                for c in reads(a, a, j):
                    c.start()

    nxt = lax.rem(g + AHEAD, SETS)

    @pl.when(g >= SETS - AHEAD)
    def _():
        for j in range(GROUP):
            for c in writes(g - (SETS - AHEAD), nxt, j):
                c.wait()

    @pl.when(g + AHEAD < n_groups)
    def _():
        for j in range(GROUP):
            for c in reads(g + AHEAD, nxt, j):
                c.start()

    cur = lax.rem(g, SETS)
    uslot = lax.rem(g, 2)

    @pl.when(g >= 2)
    def _():
        for c in u_write(g - 2, uslot):
            c.wait()

    for j in range(GROUP):
        for c in reads(g, cur, j):
            c.wait()

    for j in range(GROUP):
        local = pos[first + g * GROUP + j] - start
        b = cur * GROUP + j

        @pl.when((local >= 0) & (local < seq))
        def _():
            row0 = pl.multiple_of((local // 16) * 16, 16)
            rows = lat_buf[b, pl.ds(row0, 16), :].astype(jnp.float32)
            hit = lax.broadcasted_iota(jnp.int32, rows.shape, 0) == local - row0
            fresh = jnp.broadcast_to(lat_new[j:j + 1, :].astype(jnp.float32), rows.shape)
            lat_buf[b, pl.ds(row0, 16), :] = jnp.where(hit, fresh, rows).astype(lat_buf.dtype)
            col0 = pl.multiple_of((local // 128) * 128, 128)
            cols = rope_buf[b, :, pl.ds(col0, 128)].astype(jnp.float32)
            hit = lax.broadcasted_iota(jnp.int32, cols.shape, 1) == local - col0
            rope_buf[b, :, pl.ds(col0, 128)] = jnp.where(hit, rope_cols[:, j:j + 1], cols).astype(rope_buf.dtype)

    span = pos[first + g * GROUP] - start + 1

    def compute(width):
        lane = lax.broadcasted_iota(jnp.int32, (heads, 128), 1)
        half = g * GROUP // 128
        m_all = ml_out[0, half]
        l_all = ml_out[1, half]
        slots = lax.broadcasted_iota(jnp.int32, (heads, width), 1)

        def scores(j):
            b = cur * GROUP + j
            s = lax.dot_general(query[j, :, :rank], lat_buf[b, :width, :], (((1,), (1,)), ((), ())), preferred_element_type=jnp.float32)
            return s + jnp.dot(query[j, :, rank:rank + rope_dim], rope_buf[b, :, :width], preferred_element_type=jnp.float32)

        s_next = scores(0)
        for j in range(GROUP):
            s = s_next * score_scale
            if j + 1 < GROUP:
                s_next = scores(j + 1)
            i = g * GROUP + j
            valid = slots <= pos[first + i] - start
            s = jnp.where(valid, s, MASK_VALUE)
            m = jnp.max(s, axis=1, keepdims=True)
            w = jnp.where(valid, jnp.exp(s - m), 0.0)
            l = jnp.sum(w, axis=1, keepdims=True)
            u = jnp.dot(w.astype(jnp.bfloat16), lat_buf[cur * GROUP + j, :width, :], preferred_element_type=jnp.float32)
            for q in range(lanes):
                u_buf[uslot, q, pl.ds(j, heads, stride=GROUP), :] = u[:, q * 128:(q + 1) * 128]
            here = lane == i - half * 128
            m_all = jnp.where(here, m, m_all)
            l_all = jnp.where(here, l, l_all)
        ml_out[0, half] = m_all
        ml_out[1, half] = l_all

    widths = sorted({seq, max(seq // 2, 128), 128})
    low = 0
    for width in widths:
        cond = span > low if width == seq else (span > low) & (span <= width)

        @pl.when(cond)
        def _(width=width):
            compute(width)
        low = width

    @pl.when(span <= 0)
    def _():
        u_buf[uslot] = jnp.zeros(u_buf.shape[1:], jnp.float32)

    for j in range(GROUP):
        for c in writes(g, cur, j):
            c.start()
    for c in u_write(g, uslot):
        c.start()

    @pl.when(g == n_groups - 1)
    def _():
        for k in range(SETS - AHEAD):
            for j in range(GROUP):
                for c in writes(g - k, lax.rem(g - k, SETS), j):
                    c.wait()
        for k in range(2):
            for c in u_write(g - k, lax.rem(g - k, 2)):
                c.wait()


def attend(first, count, done, perm, pos, base, query, lat_new, rope_new, lat_cache, rope_t, score_scale):
    heads = query.shape[1]
    rank = lat_cache.shape[2]
    seq = lat_cache.shape[1]
    rope_dim = rope_t.shape[1]
    n_groups = count // GROUP
    g0 = first // GROUP
    n_ml = pl.cdiv(count, 128)
    any_spec = pl.BlockSpec(memory_space=pl.ANY)
    return pl.pallas_call(
        functools.partial(attend_kernel, score_scale, n_groups, first, len(done)),
        grid_spec=pltpu.PrefetchScalarGridSpec(
            num_scalar_prefetch=3,
            grid=(n_groups,),
            in_specs=[
                pl.BlockSpec((GROUP, heads, query.shape[2]), lambda g, *_: (g + g0, 0, 0)),
                pl.BlockSpec((GROUP, rank), lambda g, *_: (g + g0, 0)),
                pl.BlockSpec((GROUP, rope_dim), lambda g, *_: (g + g0, 0)),
            ] + [any_spec] * (2 + len(done)),
            out_specs=[any_spec, any_spec, any_spec,
                       pl.BlockSpec((2, n_ml, heads, 128), lambda g, *_: (0, 0, 0, 0))],
            scratch_shapes=[
                pltpu.VMEM((SETS * GROUP, seq, rank), jnp.bfloat16),
                pltpu.VMEM((SETS * GROUP, rope_dim, seq), jnp.bfloat16),
                pltpu.VMEM((2, rank // 128, heads * GROUP, 128), jnp.float32),
                pltpu.SemaphoreType.DMA((SETS * GROUP,)),
                pltpu.SemaphoreType.DMA((SETS * GROUP,)),
                pltpu.SemaphoreType.DMA((SETS * GROUP,)),
                pltpu.SemaphoreType.DMA((SETS * GROUP,)),
                pltpu.SemaphoreType.DMA((2, rank // 128)),
            ],
        ),
        out_shape=[
            jax.ShapeDtypeStruct(lat_cache.shape, lat_cache.dtype),
            jax.ShapeDtypeStruct(rope_t.shape, rope_t.dtype),
            jax.ShapeDtypeStruct((heads, count, rank), jnp.float32),
            jax.ShapeDtypeStruct((2, n_ml, heads, 128), jnp.float32),
        ],
        input_output_aliases={8: 0, 9: 1} if done else {},
        compiler_params=pltpu.CompilerParams(dimension_semantics=("arbitrary",), vmem_limit_bytes=48 * 1024 * 1024),
        cost_estimate=pl.CostEstimate(flops=16 * count * heads * seq * (2 * rank + rope_dim), bytes_accessed=count * seq * rank * 5,
                                      transcendentals=0),
        name=f"attend{first}_{count}",
    )(perm, pos, base, query, lat_new, rope_new, lat_cache, rope_t, *done)


CH = 4


def row_block(rows):
    return max(d for d in range(8, 65, 8) if rows % d == 0)


def remote(src, dst, ss, rs, dev):
    return pltpu.make_async_remote_copy(src_ref=src, dst_ref=dst, send_sem=ss, recv_sem=rs,
                                        device_id=dev, device_id_type=MESH)


def factors(stats, mine, other, lo, count, f_buf):
    sources = stats.shape[0]
    for b in range(stats.shape[2]):
        m = [stats[s, 0, b, pl.ds(lo, count), :] for s in range(sources)]
        top = functools.reduce(jnp.maximum, m)
        total = sum(jnp.exp(m[s] - top) * stats[s, 1, b, pl.ds(lo, count), :] for s in range(sources))
        total = jnp.maximum(total, 1e-30)
        for slot, s in enumerate((mine, other)):
            f = jnp.exp(stats[s, 0, b, pl.ds(lo, count), :] - top) / total
            f_buf[slot, b * 128:(b + 1) * 128, :] = f.T


def column(f_buf, slot, r0, rb, h):
    f = f_buf[slot, pl.ds(r0, rb), :]
    lane = lax.broadcasted_iota(jnp.int32, f.shape, 1)
    return jnp.sum(jnp.where(lane == h, f, 0.0), axis=1, keepdims=True)


def pair_kernel(u_ref, ml_ref, keep_ref, give_ref, d_buf, own_buf, stats, f_buf,
                d_ss, d_rs, s_ss, s_rs, own_sem, out_sem):
    hh, rows, rank = d_buf.shape
    half = rows // 2
    n_chunk = hh // CH
    dp = lax.axis_index('dp')
    tp = lax.axis_index('tp')
    sp = lax.axis_index('sp')
    n_sp = stats.shape[0]
    core = lax.rem(sp, 2)
    x = sp // 2
    mate = x * 2 + (1 - core)
    peers = [lax.rem(sp + i, n_sp) for i in range(1, n_sp)]
    barrier = pltpu.get_barrier_semaphore()
    for p in peers:
        pl.semaphore_signal(barrier, inc=1, device_id={'dp': dp, 'tp': tp, 'sp': p}, device_id_type=MESH)

    def own_load(k):
        return pltpu.make_async_copy(u_ref.at[pl.ds(core * hh + k * CH, CH)], own_buf.at[lax.rem(k, 2)], own_sem.at[lax.rem(k, 2)])

    for k in range(2):
        own_load(k).start()
    pl.semaphore_wait(barrier, n_sp - 1)

    def stat_send(i):
        return remote(ml_ref, stats.at[sp], s_ss.at[i], s_rs.at[sp], {'dp': dp, 'tp': tp, 'sp': peers[i]})

    def stat_recv(i):
        return remote(ml_ref, stats.at[peers[i]], s_ss.at[i], s_rs.at[peers[i]], {'dp': dp, 'tp': tp, 'sp': peers[i]})

    def d_copy(k):
        return remote(u_ref.at[pl.ds((1 - core) * hh + k * CH, CH)], d_buf.at[pl.ds(k * CH, CH)],
                      d_ss.at[k], d_rs.at[k], {'dp': dp, 'tp': tp, 'sp': mate})

    for i in range(n_sp - 1):
        stat_send(i).start()
    for k in range(n_chunk):
        d_copy(k).start()
    stats[sp] = ml_ref[...]
    for i in range(n_sp - 1):
        stat_recv(i).wait_recv()
    factors(stats, sp, mate, pl.multiple_of(core * hh, 8), hh, f_buf)

    keep = pl.multiple_of(x * half, 8)
    give = pl.multiple_of((1 - x) * half, 8)
    rb = row_block(rows)

    def outs(k):
        hs = pl.ds(k * CH, CH)
        return (pltpu.make_async_copy(d_buf.at[hs, pl.ds(keep, half), :], keep_ref.at[hs], out_sem.at[0, k]),
                pltpu.make_async_copy(d_buf.at[hs, pl.ds(give, half), :], give_ref.at[hs], out_sem.at[1, k]))

    def chunk(k, _):
        own_load(k).wait()
        d_copy(k).wait_recv()
        slot = lax.rem(k, 2)

        def scale(t, _):
            a = t // (rows // rb)
            r0 = pl.multiple_of(lax.rem(t, rows // rb) * rb, rb)
            h = k * CH + a
            fo = column(f_buf, 0, r0, rb, h)
            fm = column(f_buf, 1, r0, rb, h)
            d_buf[h, pl.ds(r0, rb), :] = fo * own_buf[slot, a, pl.ds(r0, rb), :] + fm * d_buf[h, pl.ds(r0, rb), :]
            return 0

        lax.fori_loop(0, CH * (rows // rb), scale, 0)
        for c in outs(k):
            c.start()

        @pl.when(k + 2 < n_chunk)
        def _():
            own_load(k + 2).start()
        return 0

    lax.fori_loop(0, n_chunk, chunk, 0)
    for i in range(n_sp - 1):
        stat_send(i).wait_send()

    def drain(k, _):
        d_copy(k).wait_send()
        for c in outs(k):
            c.wait()
        return 0

    lax.fori_loop(0, n_chunk, drain, 0)


def pair_reduce(cid, n_sp, u, ml):
    heads, rows, rank = u.shape
    hh = heads // 2
    n_chunk = hh // CH
    dma = pltpu.SemaphoreType.DMA
    any_spec = pl.BlockSpec(memory_space=pl.ANY)
    return pl.pallas_call(
        pair_kernel,
        in_specs=[any_spec, pl.BlockSpec(memory_space=pltpu.VMEM)],
        out_specs=[any_spec, any_spec],
        out_shape=[jax.ShapeDtypeStruct((hh, rows // 2, rank), jnp.float32)] * 2,
        scratch_shapes=[
            pltpu.VMEM((hh, rows, rank), jnp.float32),
            pltpu.VMEM((2, CH, rows, rank), jnp.float32),
            pltpu.VMEM((n_sp,) + ml.shape, jnp.float32),
            pltpu.VMEM((2, ml.shape[1] * 128, hh), jnp.float32),
            dma((n_chunk,)), dma((n_chunk,)), dma((n_sp,)), dma((n_sp,)), dma((2,)), dma((2, n_chunk)),
        ],
        compiler_params=pltpu.CompilerParams(collective_id=cid, has_side_effects=True, vmem_limit_bytes=48 * 1024 * 1024),
        cost_estimate=pl.CostEstimate(flops=2_000_000_000, bytes_accessed=20_000_000, transcendentals=0),
        name=f"pair{rows}",
    )(u, ml)


def combine_kernel(n_rest, keep_ref, got_ref, wuv_ref, wout_ref, hid_ref, sel_ref, sel_t_ref, *refs):
    if n_rest:
        u_ref, ml_ref = refs[:2]
        refs = refs[2:]
    (out_ref, att, hid_buf, out_buf, hid_sem, out_sem, keep_buf, got_buf, o_out, o_in, o_all, w_buf, p_buf, y_buf, wuv_buf,
     o_ss, o_rs, y_ss, y_rs, h_ss, h_rs, c_ss, c_rs, w_ss, w_rs,
     own_sem, keep_sem, wt_sem, wuv_sem) = refs[:29]
    if n_rest:
        d_buf, own_buf, stats, f_buf, d_ss, d_rs, s_ss, s_rs = refs[29:]
    hh, half, rank = keep_ref.shape
    r_own = half + n_rest
    vdim = wuv_buf.shape[2]
    n_chunk = hh // CH
    n_blk, _, bcol = p_buf.shape
    dp = lax.axis_index('dp')
    tp = lax.axis_index('tp')
    sp = lax.axis_index('sp')
    core = lax.rem(sp, 2)
    x = sp // 2
    to_mate = {'dp': dp, 'tp': tp, 'sp': x * 2 + (1 - core)}
    to_x = {'dp': dp, 'tp': tp, 'sp': (1 - x) * 2 + core}
    to_y = {'dp': dp, 'tp': 1 - tp, 'sp': sp}

    barrier = pltpu.get_barrier_semaphore()
    for dev in (to_mate, to_x, to_y):
        pl.semaphore_signal(barrier, inc=1, device_id=dev, device_id_type=MESH)

    def loads(k):
        slot = lax.rem(k, 2)
        hs = pl.ds(k * CH, CH)
        cs = [pltpu.make_async_copy(keep_ref.at[hs], keep_buf.at[slot], keep_sem.at[0, slot]),
              pltpu.make_async_copy(got_ref.at[hs], got_buf.at[slot], keep_sem.at[1, slot])]
        if n_rest:
            cs.append(pltpu.make_async_copy(u_ref.at[pl.ds(core * hh + k * CH, CH)], own_buf.at[slot], own_sem.at[slot]))
        return cs

    def w_load(j):
        col = pl.multiple_of(core * (n_blk * bcol) + j * bcol, 128)
        return pltpu.make_async_copy(wout_ref.at[:, pl.ds(col, bcol)], w_buf.at[lax.rem(j, 2)], wt_sem.at[lax.rem(j, 2)])

    for k in range(2):
        for c in loads(k):
            c.start()
    wuv_load = pltpu.make_async_copy(wuv_ref, wuv_buf, wuv_sem)
    wuv_load.start()
    pl.semaphore_wait(barrier, 3)

    def d_copy(k):
        return remote(u_ref.at[pl.ds((1 - core) * hh + k * CH, CH)], d_buf.at[pl.ds(k * CH, CH)],
                      d_ss.at[k], d_rs.at[k], to_mate)

    if n_rest:
        stat_copy = remote(ml_ref, stats.at[1], s_ss, s_rs, to_mate)
        stat_copy.start()
        for k in range(n_chunk):
            d_copy(k).start()
    for j in range(2):
        w_load(j).start()
    if n_rest:
        stats[0] = ml_ref[...]
        stat_copy.wait_recv()
        factors(stats, 0, 1, pl.multiple_of(core * hh, 8), hh, f_buf)

    def o_copy(k):
        return remote(o_out.at[pl.ds(k * CH, CH)], o_in.at[pl.ds(k * CH, CH)], o_ss.at[k], o_rs.at[k], to_mate)

    wuv_load.wait()
    rb = row_block(n_rest) if n_rest else 8

    def project_chunk(k, _):
        slot = lax.rem(k, 2)
        for c in loads(k):
            c.wait()
        if n_rest:
            d_copy(k).wait_recv()

            def scale(t, _):
                a = t // (n_rest // rb)
                r0 = pl.multiple_of(lax.rem(t, n_rest // rb) * rb, rb)
                h = k * CH + a
                fo = column(f_buf, 0, r0, rb, h)
                fm = column(f_buf, 1, r0, rb, h)
                d_buf[h, pl.ds(r0, rb), :] = fo * own_buf[slot, a, pl.ds(r0, rb), :] + fm * d_buf[h, pl.ds(r0, rb), :]
                return 0

            lax.fori_loop(0, CH * (n_rest // rb), scale, 0)

        def project(a, _):
            h = k * CH + a
            u = keep_buf[slot, a] + got_buf[slot, a]
            if n_rest:
                u = jnp.concatenate([u, d_buf[h]], axis=0)
            o = jnp.dot(u.astype(jnp.bfloat16), wuv_buf[h], preferred_element_type=jnp.float32).astype(jnp.bfloat16)
            o_all[:, pl.ds(pl.multiple_of((core * hh + h) * vdim, 128), vdim)] = o
            o_out[h] = o.astype(jnp.float32)
            return 0

        lax.fori_loop(0, CH, project, 0)
        o_copy(k).start()

        @pl.when(k + 2 < n_chunk)
        def _():
            for c in loads(k + 2):
                c.start()
        return 0

    lax.fori_loop(0, n_chunk, project_chunk, 0)

    def place_chunk(k, _):
        o_copy(k).wait_recv()

        def place(a, _):
            h = k * CH + a
            o_all[:, pl.ds(pl.multiple_of(((1 - core) * hh + h) * vdim, 128), vdim)] = o_in[h].astype(jnp.bfloat16)
            return 0

        lax.fori_loop(0, CH, place, 0)
        return 0

    lax.fori_loop(0, n_chunk, place_chunk, 0)

    mine = core * n_blk
    theirs = (1 - core) * n_blk

    def y_copy(j):
        return remote(p_buf.at[j], y_buf.at[j], y_ss.at[j], y_rs.at[j], to_y)

    def c_copy(j):
        return remote(att.at[x, mine + j], att.at[x, mine + j], c_ss.at[j], c_rs.at[j], to_mate)

    def h_copy(j):
        return remote(att.at[x, mine + j], att.at[x, mine + j], h_ss.at[j], h_rs.at[j], to_x)

    def w_copy(j):
        return remote(att.at[1 - x, mine + j], att.at[1 - x, mine + j], w_ss.at[j], w_rs.at[j], to_mate)

    def hid_load(kind, j):
        col = pl.multiple_of(((theirs if kind else mine) + j) * bcol, 128)
        slot = 2 * kind + lax.rem(j, 2)
        return pltpu.make_async_copy(hid_ref.at[:, pl.ds(col, bcol)], hid_buf.at[slot], hid_sem.at[slot])

    def out_store(kind, j):
        col = pl.multiple_of(((theirs if kind else mine) + j) * bcol, 128)
        slot = 2 * kind + lax.rem(j, 2)
        return pltpu.make_async_copy(out_buf.at[slot], out_ref.at[:, pl.ds(col, bcol)], out_sem.at[slot])

    def total(j):
        y_copy(j).wait_recv()
        att[x, mine + j] = y_buf[j] + p_buf[j]
        h_copy(j).start()
        c_copy(j).start()

    def forward(j):
        h_copy(j).wait_recv()
        w_copy(j).start()

    def finalize(kind, j):
        slot = 2 * kind + lax.rem(j, 2)
        blk = (theirs if kind else mine) + j
        hid_load(kind, j).wait()
        hid = jnp.dot(sel_ref[...], hid_buf[slot], preferred_element_type=jnp.float32)
        parts = [att[0, blk, :half], att[1, blk, :half]]
        if n_rest:
            parts.append(att[0, blk, half:])
        rows_s = (hid + jnp.concatenate(parts, axis=0)).astype(jnp.bfloat16)

        @pl.when(j >= 2)
        def _():
            out_store(kind, j - 2).wait()

        out_buf[slot] = jnp.dot(sel_t_ref[...], rows_s, preferred_element_type=jnp.float32).astype(out_buf.dtype)
        out_store(kind, j).start()

        @pl.when(j + 2 < n_blk)
        def _():
            hid_load(kind, j + 2).start()

    def finalize_mate(j):
        pltpu.make_async_remote_copy(src_ref=att.at[x, theirs + j], dst_ref=att.at[x, theirs + j], send_sem=c_ss.at[j],
                                     recv_sem=c_rs.at[j], device_id=to_mate, device_id_type=MESH).wait_recv()
        pltpu.make_async_remote_copy(src_ref=att.at[1 - x, theirs + j], dst_ref=att.at[1 - x, theirs + j], send_sem=w_ss.at[j],
                                     recv_sem=w_rs.at[j], device_id=to_mate, device_id_type=MESH).wait_recv()
        finalize(1, j)

    for kind in range(2):
        for j in range(2):
            hid_load(kind, j).start()
    early = (4, 8, 11)
    lag = len(early)

    def block(j, _):
        w_load(j).wait()
        p_buf[j] = jnp.dot(o_all[...], w_buf[lax.rem(j, 2)], preferred_element_type=jnp.float32)
        y_copy(j).start()

        @pl.when(j + 2 < n_blk)
        def _():
            w_load(j + 2).start()

        for i, at in enumerate(early):
            @pl.when(j == at)
            def _(i=i):
                total(i)
        return 0

    lax.fori_loop(0, n_blk, block, 0)

    def finish(j, _):
        @pl.when(j < n_blk)
        def _():
            total(j)

        @pl.when(j - lag < n_blk)
        def _():
            forward(j - lag)
            finalize(0, j - lag)

        @pl.when(j - lag >= 1)
        def _():
            finalize_mate(j - lag - 1)
        return 0

    lax.fori_loop(lag, n_blk + lag + 1, finish, 0)

    def drain(k, _):
        if n_rest:
            d_copy(k).wait_send()
        o_copy(k).wait_send()
        return 0

    lax.fori_loop(0, n_chunk, drain, 0)
    if n_rest:
        stat_copy.wait_send()

    def drain_blocks(j, _):
        y_copy(j).wait_send()
        h_copy(j).wait_send()
        c_copy(j).wait_send()
        w_copy(j).wait_send()
        return 0

    lax.fori_loop(0, n_blk, drain_blocks, 0)
    for kind in range(2):
        for j in range(n_blk - 2, n_blk):
            out_store(kind, j).wait()


def combine(cid, keep, got, wuv, wout, hidden, sel, sel_t, rest):
    hh, half, rank = keep.shape
    n_rest = rest[0].shape[1] if rest else 0
    vdim = wuv.shape[2]
    depth, width = wout.shape
    r_own = half + n_rest
    bcol = 256
    n_blk = width // 2 // bcol
    n_chunk = hh // CH
    dma = pltpu.SemaphoreType.DMA
    any_spec = pl.BlockSpec(memory_space=pl.ANY)
    vmem_spec = pl.BlockSpec(memory_space=pltpu.VMEM)
    rows = hidden.shape[0]
    scratch = [
        pltpu.VMEM((2, 2 * n_blk, r_own, bcol), jnp.float32),
        pltpu.VMEM((4, rows, bcol), jnp.bfloat16),
        pltpu.VMEM((4, rows, bcol), jnp.bfloat16),
        dma((4,)), dma((4,)),
        pltpu.VMEM((2, CH, half, rank), jnp.float32),
        pltpu.VMEM((2, CH, half, rank), jnp.float32),
        pltpu.VMEM((hh, r_own, vdim), jnp.float32),
        pltpu.VMEM((hh, r_own, vdim), jnp.float32),
        pltpu.VMEM((r_own, depth), jnp.bfloat16),
        pltpu.VMEM((2, depth, bcol), jnp.bfloat16),
        pltpu.VMEM((n_blk, r_own, bcol), jnp.float32),
        pltpu.VMEM((n_blk, r_own, bcol), jnp.float32),
        pltpu.VMEM((hh, rank, vdim), jnp.bfloat16),
    ] + [dma((n_chunk,))] * 2 + [dma((n_blk,))] * 8 + [dma((2,)), dma((2, 2)), dma((2,)), dma(())]
    if rest:
        scratch += [
            pltpu.VMEM((hh, n_rest, rank), jnp.float32),
            pltpu.VMEM((2, CH, n_rest, rank), jnp.float32),
            pltpu.VMEM((2,) + rest[1].shape, jnp.float32),
            pltpu.VMEM((2, rest[1].shape[1] * 128, hh), jnp.float32),
            dma((n_chunk,)), dma((n_chunk,)), dma(()), dma(()),
        ]
    return pl.pallas_call(
        functools.partial(combine_kernel, n_rest),
        in_specs=[any_spec] * 5 + [vmem_spec, vmem_spec] + ([any_spec, vmem_spec] if rest else []),
        out_specs=any_spec,
        out_shape=jax.ShapeDtypeStruct(hidden.shape, hidden.dtype),
        scratch_shapes=scratch,
        compiler_params=pltpu.CompilerParams(collective_id=cid, has_side_effects=True, vmem_limit_bytes=VMEM_LIMIT),
        name=f"combine{2 * half}",
    )(keep, got, wuv, wout, hidden, sel, sel_t, *rest)


def solution(mesh):
    row_spec = P('dp', None)
    cache_spec = P('dp', 'sp', None)
    head_spec = P(None, 'tp', None)
    in_specs = (row_spec, cache_spec, cache_spec, P('dp'), P(), P(), P(), P(), head_spec, head_spec, head_spec, P('tp', None))
    out_specs = (row_spec, cache_spec, cache_spec)
    n_sp = mesh.shape['sp']

    def local_step(hidden, lat_cache, rope_cache, positions, w_dq, gain_q, w_dkv, gain_kv, w_uq, w_uk, w_uv, w_out):
        rows = hidden.shape[0]
        seq = lat_cache.shape[1]
        heads = w_uk.shape[1]
        hh = heads // 2
        score_scale = YARN_MSCALE ** 2 / math.sqrt(w_uq.shape[2])
        sp = lax.axis_index('sp')
        core = lax.rem(sp, 2)

        idx = jnp.arange(rows)
        before = (positions[None, :] > positions[:, None]) | ((positions[None, :] == positions[:, None]) & (idx[None, :] < idx[:, None]))
        rank = jnp.sum(before.astype(jnp.int32), axis=1)
        sel = rank[None, :] == idx[:, None]
        perm = jnp.sum(jnp.where(sel, idx[None, :], 0), axis=1).astype(jnp.int32)
        pos_s = jnp.sum(jnp.where(sel, positions[None, :], 0), axis=1).astype(jnp.int32)
        sel16 = sel.astype(jnp.bfloat16)
        hidden_s = jnp.dot(sel16, hidden, preferred_element_type=jnp.float32).astype(jnp.bfloat16)

        query, lat_new, rope_new = project_inputs(hidden_s, pos_s, w_dq, gain_q, w_dkv, gain_kv, w_uq, w_uk)
        base = (sp * seq).astype(jnp.int32).reshape(1)
        wuv_half = lax.dynamic_slice_in_dim(w_uv, core * hh, hh, axis=1).transpose(1, 0, 2)
        rope_t = rope_cache.transpose(0, 2, 1)
        n_over = jnp.sum((positions >= (n_sp // 2) * seq).astype(jnp.int32))
        sizes = sorted({min(rows, max(16, s * rows // 256)) for s in SIZES})
        which = sum((n_over > s).astype(jnp.int32) for s in sizes[:-1])
        swap = [(i, (i + n_sp // 2) % n_sp) for i in range(n_sp)]

        def branch(n_cross, cid):
            def run(perm, pos_s, base, query, lat_new, rope_new, lat_cache, rope_t, wuv_half, w_out, hidden, sel16):
                common = (perm, pos_s, base, query, lat_new, rope_new, lat_cache, rope_t, score_scale)
                lat_out, rope_out, u_first, ml_first = attend(0, n_cross, (), *common)
                keep, give = pair_reduce(2 * cid, n_sp, u_first, ml_first)
                got = lax.ppermute(give, 'sp', swap)
                rest = ()
                if n_cross < rows:
                    lat_out, rope_out, *rest = attend(n_cross, rows - n_cross, (lat_out, rope_out), *common)
                out = combine(2 * cid + 1, keep, got, wuv_half, w_out, hidden, sel16, sel16.T, rest)
                return out, lat_out, rope_out
            return run

        out, lat_out, rope_out = lax.switch(which, [branch(s, i) for i, s in enumerate(sizes)], perm, pos_s, base, query,
                                            lat_new, rope_new, lat_cache, rope_t, wuv_half, w_out, hidden, sel16)
        return out, lat_out, rope_out.transpose(0, 2, 1)

    return jax.shard_map(local_step, mesh=mesh, in_specs=in_specs, out_specs=out_specs, check_vma=False)
```

```python
import functools
import math
import jax
import jax.numpy as jnp
from jax import lax
from jax.experimental import pallas as pl
from jax.experimental.pallas import tpu as pltpu
from jax.sharding import PartitionSpec as P

EPSILON = 1e-6
ROPE_BASE = 50000.0
YARN_MSCALE = 1.0 + 0.1 * math.log(32.0)
MASK_VALUE = -1e30
MESH = pl.DeviceIdType.MESH
GROUP = 8
SETS = 4
AHEAD = 2
UNROLL = 4
VMEM_LIMIT = 66 * 1000 * 1000
SIZES = (96, 112, 256)


def rms_norm(values, gain):
    vals32 = values.astype(jnp.float32)
    inv_rms = lax.rsqrt(jnp.mean(vals32 * vals32, axis=-1, keepdims=True) + EPSILON)
    return vals32 * inv_rms * gain.astype(jnp.float32)


def rope_tables(positions, rope_dim):
    half_dim = rope_dim // 2
    inv_freq = ROPE_BASE ** (-jnp.arange(half_dim).astype(jnp.float32) / half_dim)
    angles = positions.astype(jnp.float32)[:, None] * inv_freq[None, :]
    return jnp.cos(angles), jnp.sin(angles)


def rotate_pairs(values, cos_t, sin_t):
    half_dim = values.shape[-1] // 2
    first_half = values[..., :half_dim]
    second_half = values[..., half_dim:]
    return jnp.concatenate([first_half * cos_t - second_half * sin_t, second_half * cos_t + first_half * sin_t], axis=-1)


def query_kernel(cq, cos_t, sin_t, wq, wk, q_out, q_buf, k_buf, a_buf, r_buf):
    rows = cq.shape[0]
    heads, width, depth = wq.shape
    rank = wk.shape[0]
    nope = wk.shape[2]
    half = (width - nope) // 2
    nt = (((1,), (1,)), ((), ()))
    k_buf[...] = wk[...].astype(jnp.float32).reshape(rank * heads, nope)
    q_buf[...] = lax.dot_general(wq[...].reshape(heads * width, depth), cq[...], nt, preferred_element_type=jnp.float32)
    for h in range(heads):
        q = q_buf[h * width:(h + 1) * width, :].astype(jnp.bfloat16)
        r1 = q[nope:nope + half].astype(jnp.float32)
        r2 = q[nope + half:].astype(jnp.float32)
        r = jnp.concatenate([r1 * cos_t[...] - r2 * sin_t[...], r2 * cos_t[...] + r1 * sin_t[...],
                             jnp.zeros((128 - 2 * half, rows), jnp.float32)], axis=0)
        r_buf[pl.ds(h, rows, stride=heads), :] = r.T
        wk_h = k_buf[pl.ds(h, rank, stride=heads), :].astype(jnp.bfloat16)
        qa = lax.dot_general(q[:nope].T, wk_h, nt, preferred_element_type=jnp.float32)
        for c in range(rank // 128):
            a_buf[c, pl.ds(h, rows, stride=heads), :] = qa[:, c * 128:(c + 1) * 128]
    for c in range(rank // 128):
        q_out[:, :, c * 128:(c + 1) * 128] = a_buf[c].reshape(rows, heads, 128).astype(q_out.dtype)
    q_out[:, :, rank:] = r_buf[...].reshape(rows, heads, 128).astype(q_out.dtype)


def queries(cq, cos_w, sin_w, w_uq, w_uk):
    rows, qrank = cq.shape
    wq = w_uq.transpose(1, 2, 0)
    heads, width, _ = wq.shape
    rank, _, nope = w_uk.shape
    hb = 8
    rope_dim = width - nope
    return pl.pallas_call(
        query_kernel,
        grid=(heads // hb,),
        in_specs=[
            pl.BlockSpec((rows, qrank), lambda i: (0, 0)),
            pl.BlockSpec((rope_dim // 2, rows), lambda i: (0, 0)),
            pl.BlockSpec((rope_dim // 2, rows), lambda i: (0, 0)),
            pl.BlockSpec((hb, width, qrank), lambda i: (i, 0, 0)),
            pl.BlockSpec((rank, hb, nope), lambda i: (0, i, 0)),
        ],
        out_specs=pl.BlockSpec((rows, hb, rank + 128), lambda i: (0, i, 0)),
        out_shape=jax.ShapeDtypeStruct((rows, heads, rank + 128), jnp.bfloat16),
        scratch_shapes=[
            pltpu.VMEM((hb * width, rows), jnp.float32),
            pltpu.VMEM((rank * hb, nope), jnp.float32),
            pltpu.VMEM((rank // 128, rows * hb, 128), jnp.float32),
            pltpu.VMEM((rows * hb, 128), jnp.float32),
        ],
        compiler_params=pltpu.CompilerParams(dimension_semantics=("arbitrary",), vmem_limit_bytes=48 * 1024 * 1024),
        cost_estimate=pl.CostEstimate(flops=2 * rows * heads * (width * qrank + nope * rank), bytes_accessed=70_000_000, transcendentals=0),
        name="queries",
    )(cq, cos_w, sin_w, wq, w_uk)


def project_inputs(hidden, positions, w_dq, gain_q, w_dkv, gain_kv, w_uq, w_uk):
    kv_rank = w_uk.shape[0]
    nope_dim = w_uk.shape[2]
    cos_t, sin_t = rope_tables(positions, w_uq.shape[2] - nope_dim)
    h_q = jnp.dot(hidden, w_dq, preferred_element_type=jnp.float32).astype(jnp.bfloat16)
    c_q = rms_norm(h_q, gain_q).astype(jnp.bfloat16)
    query = queries(c_q, cos_t.T, sin_t.T, w_uq, w_uk)
    kv_down = jnp.dot(hidden, w_dkv, preferred_element_type=jnp.float32).astype(jnp.bfloat16)
    lat_new = rms_norm(kv_down[:, :kv_rank], gain_kv).astype(jnp.bfloat16)
    rope_new = rotate_pairs(kv_down[:, kv_rank:].astype(jnp.float32), cos_t, sin_t).astype(jnp.bfloat16)
    return query, lat_new, rope_new


def attend_kernel(score_scale, n_groups, first, n_alias, widths, perm, pos, base, query, lat_new, rope_new, lat_in, rope_in, *rest):
    (lat_out, rope_out, u_out, ml_out, lat_buf, rope_buf, u_buf,
     lat_rd, rope_rd, lat_wr, rope_wr, u_wr) = rest[n_alias:]
    g = pl.program_id(0)
    seq = lat_buf.shape[1]
    rank = lat_buf.shape[2]
    rope_dim = rope_buf.shape[1]
    heads = query.shape[1]
    start = base[0]
    rope_cols = rope_new[...].astype(jnp.float32).T

    def reads(group, slot, j):
        req = perm[first + group * GROUP + j]
        b = slot * GROUP + j
        return (pltpu.make_async_copy(lat_in.at[req], lat_buf.at[b], lat_rd.at[b]),
                pltpu.make_async_copy(rope_in.at[req], rope_buf.at[b], rope_rd.at[b]))

    def writes(group, slot, j):
        req = perm[first + group * GROUP + j]
        b = slot * GROUP + j
        return (pltpu.make_async_copy(lat_buf.at[b], lat_out.at[req], lat_wr.at[b]),
                pltpu.make_async_copy(rope_buf.at[b], rope_out.at[req], rope_wr.at[b]))

    lanes = u_buf.shape[1]

    def u_write(group, slot):
        return [pltpu.make_async_copy(u_buf.at[slot, q].reshape(heads, GROUP, 128),
                                      u_out.at[:, pl.ds(group * GROUP, GROUP), pl.ds(q * 128, 128)], u_wr.at[slot, q])
                for q in range(lanes)]

    @pl.when(g == 0)
    def _():
        ml_out[0] = jnp.full(ml_out.shape[1:], MASK_VALUE, jnp.float32)
        ml_out[1] = jnp.zeros(ml_out.shape[1:], jnp.float32)
        for a in range(AHEAD):
            for j in range(GROUP):
                for c in reads(a, a, j):
                    c.start()

    nxt = lax.rem(g + AHEAD, SETS)

    @pl.when(g >= SETS - AHEAD)
    def _():
        for j in range(GROUP):
            for c in writes(g - (SETS - AHEAD), nxt, j):
                c.wait()

    @pl.when(g + AHEAD < n_groups)
    def _():
        for j in range(GROUP):
            for c in reads(g + AHEAD, nxt, j):
                c.start()

    cur = lax.rem(g, SETS)
    uslot = lax.rem(g, 2)

    @pl.when(g >= 2)
    def _():
        for c in u_write(g - 2, uslot):
            c.wait()

    for j in range(GROUP):
        for c in reads(g, cur, j):
            c.wait()

    def update(j, _):
        local = pos[first + g * GROUP + j] - start
        b = cur * GROUP + j

        @pl.when((local >= 0) & (local < seq))
        def _():
            row0 = pl.multiple_of((local // 16) * 16, 16)
            rows = lat_buf[b, pl.ds(row0, 16), :].astype(jnp.float32)
            hit = lax.broadcasted_iota(jnp.int32, rows.shape, 0) == local - row0
            fresh = jnp.sum(jnp.where(lax.broadcasted_iota(jnp.int32, (GROUP, rank), 0) == j, lat_new[...].astype(jnp.float32), 0.0), axis=0, keepdims=True)
            lat_buf[b, pl.ds(row0, 16), :] = jnp.where(hit, fresh, rows).astype(lat_buf.dtype)
            col0 = pl.multiple_of((local // 128) * 128, 128)
            cols = rope_buf[b, :, pl.ds(col0, 128)].astype(jnp.float32)
            hit = lax.broadcasted_iota(jnp.int32, cols.shape, 1) == local - col0
            rope_buf[b, :, pl.ds(col0, 128)] = jnp.where(hit, jnp.sum(jnp.where(lax.broadcasted_iota(jnp.int32, rope_cols.shape, 1) == j, rope_cols, 0.0), axis=1, keepdims=True), cols).astype(rope_buf.dtype)
        return 0

    lax.fori_loop(0, GROUP, update, 0)

    span = pos[first + g * GROUP] - start + 1

    def compute(width):
        lane = lax.broadcasted_iota(jnp.int32, (heads, 128), 1)
        half = g * GROUP // 128
        m_all = ml_out[0, half]
        l_all = ml_out[1, half]
        slots = lax.broadcasted_iota(jnp.int32, (heads, width), 1)

        def scores(j):
            b = cur * GROUP + j
            s = lax.dot_general(query[j, :, :rank], lat_buf[b, :width, :], (((1,), (1,)), ((), ())), preferred_element_type=jnp.float32)
            return s + jnp.dot(query[j, :, rank:rank + rope_dim], rope_buf[b, :, :width], preferred_element_type=jnp.float32)

        def several(t, carry):
            m_all, l_all = carry
            s_next = scores(t * UNROLL)
            for jj in range(UNROLL):
                j = t * UNROLL + jj
                s = s_next * score_scale
                if jj + 1 < UNROLL:
                    s_next = scores(j + 1)
                i = g * GROUP + j
                valid = slots <= pos[first + i] - start
                s = jnp.where(valid, s, MASK_VALUE)
                m = jnp.max(s, axis=1, keepdims=True)
                w = jnp.where(valid, jnp.exp(s - m), 0.0)
                l = jnp.sum(w, axis=1, keepdims=True)
                u = jnp.dot(w.astype(jnp.bfloat16), lat_buf[cur * GROUP + j, :width, :], preferred_element_type=jnp.float32)
                for q in range(lanes):
                    u_buf[uslot, q, pl.ds(j, heads, stride=GROUP), :] = u[:, q * 128:(q + 1) * 128]
                here = lane == i - half * 128
                m_all = jnp.where(here, m, m_all)
                l_all = jnp.where(here, l, l_all)
            return m_all, l_all

        m_all, l_all = lax.fori_loop(0, GROUP // UNROLL, several, (m_all, l_all))
        ml_out[0, half] = m_all
        ml_out[1, half] = l_all

    low = 0
    for width in widths:
        cond = span > low if width == seq else (span > low) & (span <= width)

        @pl.when(cond)
        def _(width=width):
            compute(width)
        low = width

    @pl.when(span <= 0)
    def _():
        u_buf[uslot] = jnp.zeros(u_buf.shape[1:], jnp.float32)

    for j in range(GROUP):
        for c in writes(g, cur, j):
            c.start()
    for c in u_write(g, uslot):
        c.start()

    @pl.when(g == n_groups - 1)
    def _():
        for k in range(SETS - AHEAD):
            for j in range(GROUP):
                for c in writes(g - k, lax.rem(g - k, SETS), j):
                    c.wait()
        for k in range(2):
            for c in u_write(g - k, lax.rem(g - k, 2)):
                c.wait()


def attend(first, count, done, perm, pos, base, query, lat_new, rope_new, lat_cache, rope_t, score_scale):
    heads = query.shape[1]
    rank = lat_cache.shape[2]
    seq = lat_cache.shape[1]
    rope_dim = rope_t.shape[1]
    n_groups = count // GROUP
    g0 = first // GROUP
    n_ml = pl.cdiv(count, 128)
    any_spec = pl.BlockSpec(memory_space=pl.ANY)
    return pl.pallas_call(
        functools.partial(attend_kernel, score_scale, n_groups, first, len(done), (128, seq) if first or count == perm.shape[0] else (seq,)),
        grid_spec=pltpu.PrefetchScalarGridSpec(
            num_scalar_prefetch=3,
            grid=(n_groups,),
            in_specs=[
                pl.BlockSpec((GROUP, heads, query.shape[2]), lambda g, *_: (g + g0, 0, 0)),
                pl.BlockSpec((GROUP, rank), lambda g, *_: (g + g0, 0)),
                pl.BlockSpec((GROUP, rope_dim), lambda g, *_: (g + g0, 0)),
            ] + [any_spec] * (2 + len(done)),
            out_specs=[any_spec, any_spec, any_spec,
                       pl.BlockSpec((2, n_ml, heads, 128), lambda g, *_: (0, 0, 0, 0))],
            scratch_shapes=[
                pltpu.VMEM((SETS * GROUP, seq, rank), jnp.bfloat16),
                pltpu.VMEM((SETS * GROUP, rope_dim, seq), jnp.bfloat16),
                pltpu.VMEM((2, rank // 128, heads * GROUP, 128), jnp.float32),
                pltpu.SemaphoreType.DMA((SETS * GROUP,)),
                pltpu.SemaphoreType.DMA((SETS * GROUP,)),
                pltpu.SemaphoreType.DMA((SETS * GROUP,)),
                pltpu.SemaphoreType.DMA((SETS * GROUP,)),
                pltpu.SemaphoreType.DMA((2, rank // 128)),
            ],
        ),
        out_shape=[
            jax.ShapeDtypeStruct(lat_cache.shape, lat_cache.dtype),
            jax.ShapeDtypeStruct(rope_t.shape, rope_t.dtype),
            jax.ShapeDtypeStruct((heads, count, rank), jnp.float32),
            jax.ShapeDtypeStruct((2, n_ml, heads, 128), jnp.float32),
        ],
        input_output_aliases={8: 0, 9: 1} if done else {},
        compiler_params=pltpu.CompilerParams(dimension_semantics=("arbitrary",), vmem_limit_bytes=48 * 1024 * 1024),
        cost_estimate=pl.CostEstimate(flops=16 * count * heads * seq * (2 * rank + rope_dim), bytes_accessed=count * seq * rank * 5,
                                      transcendentals=0),
        name=f"attend{first}_{count}",
    )(perm, pos, base, query, lat_new, rope_new, lat_cache, rope_t, *done)


CH = 4


def row_block(rows):
    return max(d for d in range(8, 65, 8) if rows % d == 0)


def remote(src, dst, ss, rs, dev):
    return pltpu.make_async_remote_copy(src_ref=src, dst_ref=dst, send_sem=ss, recv_sem=rs,
                                        device_id=dev, device_id_type=MESH)


def factors(stats, mine, other, lo, count, f_buf):
    sources = stats.shape[0]
    for b in range(stats.shape[2]):
        m = [stats[s, 0, b, pl.ds(lo, count), :] for s in range(sources)]
        top = functools.reduce(jnp.maximum, m)
        total = sum(jnp.exp(m[s] - top) * stats[s, 1, b, pl.ds(lo, count), :] for s in range(sources))
        total = jnp.maximum(total, 1e-30)
        for slot, s in enumerate((mine, other)):
            f = jnp.exp(stats[s, 0, b, pl.ds(lo, count), :] - top) / total
            f_buf[slot, b * 128:(b + 1) * 128, :] = f.T


def column(f_buf, slot, r0, rb, h):
    f = f_buf[slot, pl.ds(r0, rb), :]
    lane = lax.broadcasted_iota(jnp.int32, f.shape, 1)
    return jnp.sum(jnp.where(lane == h, f, 0.0), axis=1, keepdims=True)


def pair_kernel(u_ref, ml_ref, keep_ref, give_ref, d_buf, own_buf, stats, f_buf,
                d_ss, d_rs, s_ss, s_rs, own_sem, out_sem):
    hh, rows, rank = d_buf.shape
    half = rows // 2
    n_chunk = hh // CH
    dp = lax.axis_index('dp')
    tp = lax.axis_index('tp')
    sp = lax.axis_index('sp')
    n_sp = stats.shape[0]
    core = lax.rem(sp, 2)
    x = sp // 2
    mate = x * 2 + (1 - core)
    peers = [lax.rem(sp + i, n_sp) for i in range(1, n_sp)]
    barrier = pltpu.get_barrier_semaphore()
    for p in peers:
        pl.semaphore_signal(barrier, inc=1, device_id={'dp': dp, 'tp': tp, 'sp': p}, device_id_type=MESH)

    def own_load(k):
        return pltpu.make_async_copy(u_ref.at[pl.ds(core * hh + k * CH, CH)], own_buf.at[lax.rem(k, 2)], own_sem.at[lax.rem(k, 2)])

    for k in range(2):
        own_load(k).start()
    pl.semaphore_wait(barrier, n_sp - 1)

    def stat_send(i):
        return remote(ml_ref, stats.at[sp], s_ss.at[i], s_rs.at[sp], {'dp': dp, 'tp': tp, 'sp': peers[i]})

    def stat_recv(i):
        return remote(ml_ref, stats.at[peers[i]], s_ss.at[i], s_rs.at[peers[i]], {'dp': dp, 'tp': tp, 'sp': peers[i]})

    def d_copy(k):
        return remote(u_ref.at[pl.ds((1 - core) * hh + k * CH, CH)], d_buf.at[pl.ds(k * CH, CH)],
                      d_ss.at[k], d_rs.at[k], {'dp': dp, 'tp': tp, 'sp': mate})

    for i in range(n_sp - 1):
        stat_send(i).start()
    for k in range(n_chunk):
        d_copy(k).start()
    stats[sp] = ml_ref[...]
    for i in range(n_sp - 1):
        stat_recv(i).wait_recv()
    factors(stats, sp, mate, pl.multiple_of(core * hh, 8), hh, f_buf)

    keep = pl.multiple_of(x * half, 8)
    give = pl.multiple_of((1 - x) * half, 8)
    rb = row_block(rows)

    def outs(k):
        hs = pl.ds(k * CH, CH)
        return (pltpu.make_async_copy(d_buf.at[hs, pl.ds(keep, half), :], keep_ref.at[hs], out_sem.at[0, k]),
                pltpu.make_async_copy(d_buf.at[hs, pl.ds(give, half), :], give_ref.at[hs], out_sem.at[1, k]))

    def chunk(k, _):
        own_load(k).wait()
        d_copy(k).wait_recv()
        slot = lax.rem(k, 2)

        def scale(t, _):
            a = t // (rows // rb)
            r0 = pl.multiple_of(lax.rem(t, rows // rb) * rb, rb)
            h = k * CH + a
            fo = column(f_buf, 0, r0, rb, h)
            fm = column(f_buf, 1, r0, rb, h)
            d_buf[h, pl.ds(r0, rb), :] = fo * own_buf[slot, a, pl.ds(r0, rb), :] + fm * d_buf[h, pl.ds(r0, rb), :]
            return 0

        lax.fori_loop(0, CH * (rows // rb), scale, 0)
        for c in outs(k):
            c.start()

        @pl.when(k + 2 < n_chunk)
        def _():
            own_load(k + 2).start()
        return 0

    lax.fori_loop(0, n_chunk, chunk, 0)
    for i in range(n_sp - 1):
        stat_send(i).wait_send()

    def drain(k, _):
        d_copy(k).wait_send()
        for c in outs(k):
            c.wait()
        return 0

    lax.fori_loop(0, n_chunk, drain, 0)


def pair_reduce(cid, n_sp, u, ml):
    heads, rows, rank = u.shape
    hh = heads // 2
    n_chunk = hh // CH
    dma = pltpu.SemaphoreType.DMA
    any_spec = pl.BlockSpec(memory_space=pl.ANY)
    return pl.pallas_call(
        pair_kernel,
        in_specs=[any_spec, pl.BlockSpec(memory_space=pltpu.VMEM)],
        out_specs=[any_spec, any_spec],
        out_shape=[jax.ShapeDtypeStruct((hh, rows // 2, rank), jnp.float32)] * 2,
        scratch_shapes=[
            pltpu.VMEM((hh, rows, rank), jnp.float32),
            pltpu.VMEM((2, CH, rows, rank), jnp.float32),
            pltpu.VMEM((n_sp,) + ml.shape, jnp.float32),
            pltpu.VMEM((2, ml.shape[1] * 128, hh), jnp.float32),
            dma((n_chunk,)), dma((n_chunk,)), dma((n_sp,)), dma((n_sp,)), dma((2,)), dma((2, n_chunk)),
        ],
        compiler_params=pltpu.CompilerParams(collective_id=cid, has_side_effects=True, vmem_limit_bytes=48 * 1024 * 1024),
        cost_estimate=pl.CostEstimate(flops=2_000_000_000, bytes_accessed=20_000_000, transcendentals=0),
        name=f"pair{rows}",
    )(u, ml)


def combine_kernel(n_rest, keep_ref, got_ref, wuv_ref, wout_ref, hid_ref, sel_ref, sel_t_ref, *refs):
    if n_rest:
        u_ref, ml_ref = refs[:2]
        refs = refs[2:]
    (out_ref, att, hid_buf, out_buf, hid_sem, out_sem, keep_buf, got_buf, o_out, o_in, o_all, w_buf, p_buf, y_buf, wuv_buf, k_buf,
     o_ss, o_rs, y_ss, y_rs, h_ss, h_rs, c_ss, c_rs, w_ss, w_rs,
     own_sem, keep_sem, wt_sem, wuv_sem) = refs[:30]
    if n_rest:
        d_buf, own_buf, stats, f_buf, d_ss, d_rs, s_ss, s_rs = refs[30:]
    hh, half, rank = keep_ref.shape
    r_own = half + n_rest
    vdim = wuv_buf.shape[3]
    wh = wuv_buf.shape[2]
    n_chunk = hh // CH
    n_blk, _, bcol = p_buf.shape
    dp = lax.axis_index('dp')
    tp = lax.axis_index('tp')
    sp = lax.axis_index('sp')
    core = lax.rem(sp, 2)
    x = sp // 2
    to_mate = {'dp': dp, 'tp': tp, 'sp': x * 2 + (1 - core)}
    to_x = {'dp': dp, 'tp': tp, 'sp': (1 - x) * 2 + core}
    to_y = {'dp': dp, 'tp': 1 - tp, 'sp': sp}

    barrier = pltpu.get_barrier_semaphore()
    for dev in (to_mate, to_x, to_y):
        pl.semaphore_signal(barrier, inc=1, device_id=dev, device_id_type=MESH)

    def loads(k):
        slot = lax.rem(k, 2)
        hs = pl.ds(k * CH, CH)
        cs = [pltpu.make_async_copy(keep_ref.at[hs], keep_buf.at[slot], keep_sem.at[0, slot]),
              pltpu.make_async_copy(got_ref.at[hs], got_buf.at[slot], keep_sem.at[1, slot])]
        if n_rest:
            cs.append(pltpu.make_async_copy(u_ref.at[pl.ds(core * hh + k * CH, CH)], own_buf.at[slot], own_sem.at[slot]))
        return cs

    def w_load(j):
        col = pl.multiple_of(core * (n_blk * bcol) + j * bcol, 128)
        return pltpu.make_async_copy(wout_ref.at[:, pl.ds(col, bcol)], w_buf.at[lax.rem(j, 2)], wt_sem.at[lax.rem(j, 2)])

    for k in range(2):
        for c in loads(k):
            c.start()

    def wuv_load(a):
        return pltpu.make_async_copy(wuv_ref.at[:, pl.ds(core * hh + a * wh, wh), :], wuv_buf.at[a], wuv_sem.at[a])

    for a in range(hh // wh):
        wuv_load(a).start()
    pl.semaphore_wait(barrier, 3)

    def d_copy(k):
        return remote(u_ref.at[pl.ds((1 - core) * hh + k * CH, CH)], d_buf.at[pl.ds(k * CH, CH)],
                      d_ss.at[k], d_rs.at[k], to_mate)

    if n_rest:
        stat_copy = remote(ml_ref, stats.at[1], s_ss, s_rs, to_mate)
        stat_copy.start()
        for k in range(n_chunk):
            d_copy(k).start()
    for j in range(2):
        w_load(j).start()
    if n_rest:
        stats[0] = ml_ref[...]
        stat_copy.wait_recv()
        factors(stats, 0, 1, pl.multiple_of(core * hh, 8), hh, f_buf)

    def o_copy(k):
        return remote(o_out.at[pl.ds(k * CH, CH)], o_in.at[pl.ds(k * CH, CH)], o_ss.at[k], o_rs.at[k], to_mate)

    rb = row_block(n_rest) if n_rest else 8

    def project_chunk(k, _):
        slot = lax.rem(k, 2)
        for c in loads(k):
            c.wait()
        if n_rest:
            d_copy(k).wait_recv()

            def scale(t, _):
                a = t // (n_rest // rb)
                r0 = pl.multiple_of(lax.rem(t, n_rest // rb) * rb, rb)
                h = k * CH + a
                fo = column(f_buf, 0, r0, rb, h)
                fm = column(f_buf, 1, r0, rb, h)
                d_buf[h, pl.ds(r0, rb), :] = fo * own_buf[slot, a, pl.ds(r0, rb), :] + fm * d_buf[h, pl.ds(r0, rb), :]
                return 0

            lax.fori_loop(0, CH * (n_rest // rb), scale, 0)

        @pl.when(lax.rem(k, wh // CH) == 0)
        def _():
            wuv_load(k // (wh // CH)).wait()
            k_buf[...] = wuv_buf[k // (wh // CH)].astype(jnp.float32).reshape(k_buf.shape)

        def project(a, _):
            h = k * CH + a
            wuv_h = k_buf[pl.ds(lax.rem(h, wh), rank, stride=wh), :].astype(jnp.bfloat16)
            u = keep_buf[slot, a] + got_buf[slot, a]
            if n_rest:
                u = jnp.concatenate([u, d_buf[h]], axis=0)
            o = jnp.dot(u.astype(jnp.bfloat16), wuv_h, preferred_element_type=jnp.float32).astype(jnp.bfloat16)
            o_all[:, pl.ds(pl.multiple_of((core * hh + h) * vdim, 128), vdim)] = o
            o_out[h] = o.astype(jnp.float32)
            return 0

        lax.fori_loop(0, CH, project, 0)
        o_copy(k).start()

        @pl.when(k + 2 < n_chunk)
        def _():
            for c in loads(k + 2):
                c.start()
        return 0

    lax.fori_loop(0, n_chunk, project_chunk, 0)

    def place_chunk(k, _):
        o_copy(k).wait_recv()

        def place(a, _):
            h = k * CH + a
            o_all[:, pl.ds(pl.multiple_of(((1 - core) * hh + h) * vdim, 128), vdim)] = o_in[h].astype(jnp.bfloat16)
            return 0

        lax.fori_loop(0, CH, place, 0)
        return 0

    lax.fori_loop(0, n_chunk, place_chunk, 0)

    mine = core * n_blk
    theirs = (1 - core) * n_blk

    def y_copy(j):
        return remote(p_buf.at[j], y_buf.at[j], y_ss.at[j], y_rs.at[j], to_y)

    def c_copy(j):
        return remote(att.at[x, mine + j], att.at[x, mine + j], c_ss.at[j], c_rs.at[j], to_mate)

    def h_copy(j):
        return remote(att.at[x, mine + j], att.at[x, mine + j], h_ss.at[j], h_rs.at[j], to_x)

    def w_copy(j):
        return remote(att.at[1 - x, mine + j], att.at[1 - x, mine + j], w_ss.at[j], w_rs.at[j], to_mate)

    def hid_load(kind, j):
        col = pl.multiple_of(((theirs if kind else mine) + j) * bcol, 128)
        slot = 2 * kind + lax.rem(j, 2)
        return pltpu.make_async_copy(hid_ref.at[:, pl.ds(col, bcol)], hid_buf.at[slot], hid_sem.at[slot])

    def out_store(kind, j):
        col = pl.multiple_of(((theirs if kind else mine) + j) * bcol, 128)
        slot = 2 * kind + lax.rem(j, 2)
        return pltpu.make_async_copy(out_buf.at[slot], out_ref.at[:, pl.ds(col, bcol)], out_sem.at[slot])

    def total(j):
        y_copy(j).wait_recv()
        att[x, mine + j] = y_buf[j] + p_buf[j]
        h_copy(j).start()
        c_copy(j).start()

    def forward(j):
        h_copy(j).wait_recv()
        w_copy(j).start()

    def finalize(kind, j):
        slot = 2 * kind + lax.rem(j, 2)
        blk = (theirs if kind else mine) + j
        hid_load(kind, j).wait()
        hid = jnp.dot(sel_ref[...], hid_buf[slot], preferred_element_type=jnp.float32)
        parts = [att[0, blk, :half], att[1, blk, :half]]
        if n_rest:
            parts.append(att[0, blk, half:])
        rows_s = (hid + jnp.concatenate(parts, axis=0)).astype(jnp.bfloat16)

        @pl.when(j >= 2)
        def _():
            out_store(kind, j - 2).wait()

        out_buf[slot] = jnp.dot(sel_t_ref[...], rows_s, preferred_element_type=jnp.float32).astype(out_buf.dtype)
        out_store(kind, j).start()

        @pl.when(j + 2 < n_blk)
        def _():
            hid_load(kind, j + 2).start()

    def finalize_mate(j):
        pltpu.make_async_remote_copy(src_ref=att.at[x, theirs + j], dst_ref=att.at[x, theirs + j], send_sem=c_ss.at[j],
                                     recv_sem=c_rs.at[j], device_id=to_mate, device_id_type=MESH).wait_recv()
        pltpu.make_async_remote_copy(src_ref=att.at[1 - x, theirs + j], dst_ref=att.at[1 - x, theirs + j], send_sem=w_ss.at[j],
                                     recv_sem=w_rs.at[j], device_id=to_mate, device_id_type=MESH).wait_recv()
        finalize(1, j)

    for kind in range(2):
        for j in range(2):
            hid_load(kind, j).start()
    early = (4, 8, 11)
    lag = len(early)

    def block(j, _):
        w_load(j).wait()
        p_buf[j] = jnp.dot(o_all[...], w_buf[lax.rem(j, 2)], preferred_element_type=jnp.float32)
        y_copy(j).start()

        @pl.when(j + 2 < n_blk)
        def _():
            w_load(j + 2).start()

        for i, at in enumerate(early):
            @pl.when(j == at)
            def _(i=i):
                total(i)
        return 0

    lax.fori_loop(0, n_blk, block, 0)

    def finish(j, _):
        @pl.when(j < n_blk)
        def _():
            total(j)

        @pl.when(j - lag < n_blk)
        def _():
            forward(j - lag)
            finalize(0, j - lag)

        @pl.when(j - lag >= 1)
        def _():
            finalize_mate(j - lag - 1)
        return 0

    lax.fori_loop(lag, n_blk + lag + 1, finish, 0)

    def drain(k, _):
        if n_rest:
            d_copy(k).wait_send()
        o_copy(k).wait_send()
        return 0

    lax.fori_loop(0, n_chunk, drain, 0)
    if n_rest:
        stat_copy.wait_send()

    def drain_blocks(j, _):
        y_copy(j).wait_send()
        h_copy(j).wait_send()
        c_copy(j).wait_send()
        w_copy(j).wait_send()
        return 0

    lax.fori_loop(0, n_blk, drain_blocks, 0)
    for kind in range(2):
        for j in range(n_blk - 2, n_blk):
            out_store(kind, j).wait()


def combine(cid, keep, got, wuv, wout, hidden, sel, sel_t, rest):
    hh, half, rank = keep.shape
    n_rest = rest[0].shape[1] if rest else 0
    vdim = wuv.shape[2]
    depth, width = wout.shape
    r_own = half + n_rest
    bcol = 256
    n_blk = width // 2 // bcol
    n_chunk = hh // CH
    dma = pltpu.SemaphoreType.DMA
    any_spec = pl.BlockSpec(memory_space=pl.ANY)
    vmem_spec = pl.BlockSpec(memory_space=pltpu.VMEM)
    rows = hidden.shape[0]
    scratch = [
        pltpu.VMEM((2, 2 * n_blk, r_own, bcol), jnp.float32),
        pltpu.VMEM((4, rows, bcol), jnp.bfloat16),
        pltpu.VMEM((4, rows, bcol), jnp.bfloat16),
        dma((4,)), dma((4,)),
        pltpu.VMEM((2, CH, half, rank), jnp.float32),
        pltpu.VMEM((2, CH, half, rank), jnp.float32),
        pltpu.VMEM((hh, r_own, vdim), jnp.float32),
        pltpu.VMEM((hh, r_own, vdim), jnp.float32),
        pltpu.VMEM((r_own, depth), jnp.bfloat16),
        pltpu.VMEM((2, depth, bcol), jnp.bfloat16),
        pltpu.VMEM((n_blk, r_own, bcol), jnp.float32),
        pltpu.VMEM((n_blk, r_own, bcol), jnp.float32),
        pltpu.VMEM((hh // 8, rank, 8, vdim), jnp.bfloat16),
        pltpu.VMEM((rank * 8, vdim), jnp.float32),
    ] + [dma((n_chunk,))] * 2 + [dma((n_blk,))] * 8 + [dma((2,)), dma((2, 2)), dma((2,)), dma((hh // 8,))]
    if rest:
        scratch += [
            pltpu.VMEM((hh, n_rest, rank), jnp.float32),
            pltpu.VMEM((2, CH, n_rest, rank), jnp.float32),
            pltpu.VMEM((2,) + rest[1].shape, jnp.float32),
            pltpu.VMEM((2, rest[1].shape[1] * 128, hh), jnp.float32),
            dma((n_chunk,)), dma((n_chunk,)), dma(()), dma(()),
        ]
    return pl.pallas_call(
        functools.partial(combine_kernel, n_rest),
        in_specs=[any_spec] * 5 + [vmem_spec, vmem_spec] + ([any_spec, vmem_spec] if rest else []),
        out_specs=any_spec,
        out_shape=jax.ShapeDtypeStruct(hidden.shape, hidden.dtype),
        scratch_shapes=scratch,
        compiler_params=pltpu.CompilerParams(collective_id=cid, has_side_effects=True, vmem_limit_bytes=VMEM_LIMIT),
        name=f"combine{2 * half}",
    )(keep, got, wuv, wout, hidden, sel, sel_t, *rest)


def solution(mesh):
    row_spec = P('dp', None)
    cache_spec = P('dp', 'sp', None)
    head_spec = P(None, 'tp', None)
    in_specs = (row_spec, cache_spec, cache_spec, P('dp'), P(), P(), P(), P(), head_spec, head_spec, head_spec, P('tp', None))
    out_specs = (row_spec, cache_spec, cache_spec)
    n_sp = mesh.shape['sp']

    def local_step(hidden, lat_cache, rope_cache, positions, w_dq, gain_q, w_dkv, gain_kv, w_uq, w_uk, w_uv, w_out):
        rows = hidden.shape[0]
        seq = lat_cache.shape[1]
        heads = w_uk.shape[1]
        score_scale = YARN_MSCALE ** 2 / math.sqrt(w_uq.shape[2])
        sp = lax.axis_index('sp')

        idx = jnp.arange(rows)
        before = (positions[None, :] > positions[:, None]) | ((positions[None, :] == positions[:, None]) & (idx[None, :] < idx[:, None]))
        rank = jnp.sum(before.astype(jnp.int32), axis=1)
        sel = rank[None, :] == idx[:, None]
        perm = jnp.sum(jnp.where(sel, idx[None, :], 0), axis=1).astype(jnp.int32)
        pos_s = jnp.sum(jnp.where(sel, positions[None, :], 0), axis=1).astype(jnp.int32)
        sel16 = sel.astype(jnp.bfloat16)
        hidden_s = jnp.dot(sel16, hidden, preferred_element_type=jnp.float32).astype(jnp.bfloat16)

        query, lat_new, rope_new = project_inputs(hidden_s, pos_s, w_dq, gain_q, w_dkv, gain_kv, w_uq, w_uk)
        base = (sp * seq).astype(jnp.int32).reshape(1)
        rope_t = rope_cache.transpose(0, 2, 1)
        n_over = jnp.sum((positions >= (n_sp // 2) * seq).astype(jnp.int32))
        sizes = sorted({min(rows, max(16, s * rows // 256)) for s in SIZES})
        which = sum((n_over > s).astype(jnp.int32) for s in sizes[:-1])
        swap = [(i, (i + n_sp // 2) % n_sp) for i in range(n_sp)]

        def branch(n_cross, cid):
            def run(perm, pos_s, base, query, lat_new, rope_new, lat_cache, rope_t, w_uv, w_out, hidden, sel16):
                common = (perm, pos_s, base, query, lat_new, rope_new, lat_cache, rope_t, score_scale)
                lat_out, rope_out, u_first, ml_first = attend(0, n_cross, (), *common)
                keep, give = pair_reduce(2 * cid, n_sp, u_first, ml_first)
                got = lax.ppermute(give, 'sp', swap)
                rest = ()
                if n_cross < rows:
                    lat_out, rope_out, *rest = attend(n_cross, rows - n_cross, (lat_out, rope_out), *common)
                out = combine(2 * cid + 1, keep, got, w_uv, w_out, hidden, sel16, sel16.T, rest)
                return out, lat_out, rope_out
            return run

        out, lat_out, rope_out = lax.switch(which, [branch(s, i) for i, s in enumerate(sizes)], perm, pos_s, base, query,
                                            lat_new, rope_new, lat_cache, rope_t, w_uv, w_out, hidden, sel16)
        return out, lat_out, rope_out.transpose(0, 2, 1)

    return jax.shard_map(local_step, mesh=mesh, in_specs=in_specs, out_specs=out_specs, check_vma=False)
```

```python
import functools
import math
import jax
import jax.numpy as jnp
from jax import lax
from jax.experimental import pallas as pl
from jax.experimental.pallas import tpu as pltpu
from jax.sharding import PartitionSpec as P

EPSILON = 1e-6
ROPE_BASE = 50000.0
YARN_MSCALE = 1.0 + 0.1 * math.log(32.0)
MASK_VALUE = -1e30
MESH = pl.DeviceIdType.MESH
GROUP = 8
SETS = 4
AHEAD = 2
UNROLL = 4
VMEM_LIMIT = 66 * 1000 * 1000
SIZES = (96, 112, 256)


def rms_norm(values, gain):
    vals32 = values.astype(jnp.float32)
    inv_rms = lax.rsqrt(jnp.mean(vals32 * vals32, axis=-1, keepdims=True) + EPSILON)
    return vals32 * inv_rms * gain.astype(jnp.float32)


def rope_tables(positions, rope_dim):
    half_dim = rope_dim // 2
    inv_freq = ROPE_BASE ** (-jnp.arange(half_dim).astype(jnp.float32) / half_dim)
    angles = positions.astype(jnp.float32)[:, None] * inv_freq[None, :]
    return jnp.cos(angles), jnp.sin(angles)


def rotate_pairs(values, cos_t, sin_t):
    half_dim = values.shape[-1] // 2
    first_half = values[..., :half_dim]
    second_half = values[..., half_dim:]
    return jnp.concatenate([first_half * cos_t - second_half * sin_t, second_half * cos_t + first_half * sin_t], axis=-1)


def query_kernel(cq, cos_t, sin_t, wq, wk, q_out, q_buf, q2_buf, k_buf, a_buf, r_buf):
    rows = cq.shape[0]
    heads, width, depth = wq.shape
    rank = wk.shape[0]
    nope = wk.shape[2]
    half = (width - nope) // 2
    nt = (((1,), (1,)), ((), ()))
    k_buf[...] = wk[...].astype(jnp.float32).reshape(rank * heads, nope)
    part = heads // 2
    for a, buf in enumerate((q_buf, q2_buf)):
        buf[...] = lax.dot_general(wq[a * part:(a + 1) * part].reshape(part * width, depth), cq[...], nt, preferred_element_type=jnp.float32)
    for h in range(heads):
        buf = (q_buf, q2_buf)[h // part]
        q = buf[(h % part) * width:(h % part + 1) * width, :].astype(jnp.bfloat16)
        r1 = q[nope:nope + half].astype(jnp.float32)
        r2 = q[nope + half:].astype(jnp.float32)
        r = jnp.concatenate([r1 * cos_t[...] - r2 * sin_t[...], r2 * cos_t[...] + r1 * sin_t[...],
                             jnp.zeros((128 - 2 * half, rows), jnp.float32)], axis=0)
        r_buf[pl.ds(h, rows, stride=heads), :] = r.T
        wk_h = k_buf[pl.ds(h, rank, stride=heads), :].astype(jnp.bfloat16)
        qa = lax.dot_general(q[:nope].T, wk_h, nt, preferred_element_type=jnp.float32)
        for c in range(rank // 128):
            a_buf[c, pl.ds(h, rows, stride=heads), :] = qa[:, c * 128:(c + 1) * 128]
    for c in range(rank // 128):
        q_out[:, :, c * 128:(c + 1) * 128] = a_buf[c].reshape(rows, heads, 128).astype(q_out.dtype)
    q_out[:, :, rank:] = r_buf[...].reshape(rows, heads, 128).astype(q_out.dtype)


def queries(cq, cos_w, sin_w, w_uq, w_uk):
    rows, qrank = cq.shape
    wq = w_uq.transpose(1, 2, 0)
    heads, width, _ = wq.shape
    rank, _, nope = w_uk.shape
    hb = 8
    rope_dim = width - nope
    return pl.pallas_call(
        query_kernel,
        grid=(heads // hb,),
        in_specs=[
            pl.BlockSpec((rows, qrank), lambda i: (0, 0)),
            pl.BlockSpec((rope_dim // 2, rows), lambda i: (0, 0)),
            pl.BlockSpec((rope_dim // 2, rows), lambda i: (0, 0)),
            pl.BlockSpec((hb, width, qrank), lambda i: (i, 0, 0)),
            pl.BlockSpec((rank, hb, nope), lambda i: (0, i, 0)),
        ],
        out_specs=pl.BlockSpec((rows, hb, rank + 128), lambda i: (0, i, 0)),
        out_shape=jax.ShapeDtypeStruct((rows, heads, rank + 128), jnp.bfloat16),
        scratch_shapes=[
            pltpu.VMEM((hb * width // 2, rows), jnp.float32),
            pltpu.VMEM((hb * width // 2, rows), jnp.float32),
            pltpu.VMEM((rank * hb, nope), jnp.float32),
            pltpu.VMEM((rank // 128, rows * hb, 128), jnp.float32),
            pltpu.VMEM((rows * hb, 128), jnp.float32),
        ],
        compiler_params=pltpu.CompilerParams(dimension_semantics=("arbitrary",), vmem_limit_bytes=48 * 1024 * 1024),
        cost_estimate=pl.CostEstimate(flops=2 * rows * heads * (width * qrank + nope * rank), bytes_accessed=70_000_000, transcendentals=0),
        name="queries",
    )(cq, cos_w, sin_w, wq, w_uk)


def project_inputs(hidden, positions, w_dq, gain_q, w_dkv, gain_kv, w_uq, w_uk):
    kv_rank = w_uk.shape[0]
    nope_dim = w_uk.shape[2]
    cos_t, sin_t = rope_tables(positions, w_uq.shape[2] - nope_dim)
    h_q = jnp.dot(hidden, w_dq, preferred_element_type=jnp.float32).astype(jnp.bfloat16)
    c_q = rms_norm(h_q, gain_q).astype(jnp.bfloat16)
    query = queries(c_q, cos_t.T, sin_t.T, w_uq, w_uk)
    kv_down = jnp.dot(hidden, w_dkv, preferred_element_type=jnp.float32).astype(jnp.bfloat16)
    lat_new = rms_norm(kv_down[:, :kv_rank], gain_kv).astype(jnp.bfloat16)
    rope_new = rotate_pairs(kv_down[:, kv_rank:].astype(jnp.float32), cos_t, sin_t).astype(jnp.bfloat16)
    return query, lat_new, rope_new


def attend_kernel(score_scale, n_groups, first, n_alias, widths, perm, pos, base, query, lat_new, rope_new, lat_in, rope_in, *rest):
    (lat_out, rope_out, u_out, ml_out, lat_buf, rope_buf, u_buf,
     lat_rd, rope_rd, lat_wr, rope_wr, u_wr) = rest[n_alias:]
    g = pl.program_id(0)
    seq = lat_buf.shape[1]
    rank = lat_buf.shape[2]
    rope_dim = rope_buf.shape[1]
    heads = query.shape[1]
    start = base[0]
    rope_cols = rope_new[...].astype(jnp.float32).T

    def reads(group, slot, j):
        req = perm[first + group * GROUP + j]
        b = slot * GROUP + j
        return (pltpu.make_async_copy(lat_in.at[req], lat_buf.at[b], lat_rd.at[b]),
                pltpu.make_async_copy(rope_in.at[req], rope_buf.at[b], rope_rd.at[b]))

    def writes(group, slot, j):
        req = perm[first + group * GROUP + j]
        b = slot * GROUP + j
        return (pltpu.make_async_copy(lat_buf.at[b], lat_out.at[req], lat_wr.at[b]),
                pltpu.make_async_copy(rope_buf.at[b], rope_out.at[req], rope_wr.at[b]))

    lanes = u_buf.shape[1]

    def u_write(group, slot):
        return [pltpu.make_async_copy(u_buf.at[slot, q].reshape(heads, GROUP, 128),
                                      u_out.at[:, pl.ds(group * GROUP, GROUP), pl.ds(q * 128, 128)], u_wr.at[slot, q])
                for q in range(lanes)]

    @pl.when(g == 0)
    def _():
        ml_out[0] = jnp.full(ml_out.shape[1:], MASK_VALUE, jnp.float32)
        ml_out[1] = jnp.zeros(ml_out.shape[1:], jnp.float32)
        for a in range(AHEAD):
            for j in range(GROUP):
                for c in reads(a, a, j):
                    c.start()

    nxt = lax.rem(g + AHEAD, SETS)

    @pl.when(g >= SETS - AHEAD)
    def _():
        for j in range(GROUP):
            for c in writes(g - (SETS - AHEAD), nxt, j):
                c.wait()

    @pl.when(g + AHEAD < n_groups)
    def _():
        for j in range(GROUP):
            for c in reads(g + AHEAD, nxt, j):
                c.start()

    cur = lax.rem(g, SETS)
    uslot = lax.rem(g, 2)

    @pl.when(g >= 2)
    def _():
        for c in u_write(g - 2, uslot):
            c.wait()

    for j in range(GROUP):
        for c in reads(g, cur, j):
            c.wait()

    def update(j, _):
        local = pos[first + g * GROUP + j] - start
        b = cur * GROUP + j

        @pl.when((local >= 0) & (local < seq))
        def _():
            row0 = pl.multiple_of((local // 16) * 16, 16)
            rows = lat_buf[b, pl.ds(row0, 16), :].astype(jnp.float32)
            hit = lax.broadcasted_iota(jnp.int32, rows.shape, 0) == local - row0
            fresh = jnp.sum(jnp.where(lax.broadcasted_iota(jnp.int32, (GROUP, rank), 0) == j, lat_new[...].astype(jnp.float32), 0.0), axis=0, keepdims=True)
            lat_buf[b, pl.ds(row0, 16), :] = jnp.where(hit, fresh, rows).astype(lat_buf.dtype)
            col0 = pl.multiple_of((local // 128) * 128, 128)
            cols = rope_buf[b, :, pl.ds(col0, 128)].astype(jnp.float32)
            hit = lax.broadcasted_iota(jnp.int32, cols.shape, 1) == local - col0
            rope_buf[b, :, pl.ds(col0, 128)] = jnp.where(hit, jnp.sum(jnp.where(lax.broadcasted_iota(jnp.int32, rope_cols.shape, 1) == j, rope_cols, 0.0), axis=1, keepdims=True), cols).astype(rope_buf.dtype)
        return 0

    lax.fori_loop(0, GROUP, update, 0)

    span = pos[first + g * GROUP] - start + 1

    def compute(width):
        lane = lax.broadcasted_iota(jnp.int32, (heads, 128), 1)
        half = g * GROUP // 128
        m_all = ml_out[0, half]
        l_all = ml_out[1, half]
        slots = lax.broadcasted_iota(jnp.int32, (heads, width), 1)

        def scores(j):
            b = cur * GROUP + j
            s = lax.dot_general(query[j, :, :rank], lat_buf[b, :width, :], (((1,), (1,)), ((), ())), preferred_element_type=jnp.float32)
            return s + jnp.dot(query[j, :, rank:rank + rope_dim], rope_buf[b, :, :width], preferred_element_type=jnp.float32)

        def several(t, carry):
            m_all, l_all = carry
            s_next = scores(t * UNROLL)
            for jj in range(UNROLL):
                j = t * UNROLL + jj
                s = s_next * score_scale
                if jj + 1 < UNROLL:
                    s_next = scores(j + 1)
                i = g * GROUP + j
                valid = slots <= pos[first + i] - start
                s = jnp.where(valid, s, MASK_VALUE)
                m = jnp.max(s, axis=1, keepdims=True)
                w = jnp.where(valid, jnp.exp(s - m), 0.0)
                l = jnp.sum(w, axis=1, keepdims=True)
                u = jnp.dot(w.astype(jnp.bfloat16), lat_buf[cur * GROUP + j, :width, :], preferred_element_type=jnp.float32)
                for q in range(lanes):
                    u_buf[uslot, q, pl.ds(j, heads, stride=GROUP), :] = u[:, q * 128:(q + 1) * 128]
                here = lane == i - half * 128
                m_all = jnp.where(here, m, m_all)
                l_all = jnp.where(here, l, l_all)
            return m_all, l_all

        m_all, l_all = lax.fori_loop(0, GROUP // UNROLL, several, (m_all, l_all))
        ml_out[0, half] = m_all
        ml_out[1, half] = l_all

    low = 0
    for width in widths:
        cond = span > low if width == seq else (span > low) & (span <= width)

        @pl.when(cond)
        def _(width=width):
            compute(width)
        low = width

    @pl.when(span <= 0)
    def _():
        u_buf[uslot] = jnp.zeros(u_buf.shape[1:], jnp.float32)

    for j in range(GROUP):
        for c in writes(g, cur, j):
            c.start()
    for c in u_write(g, uslot):
        c.start()

    @pl.when(g == n_groups - 1)
    def _():
        for k in range(SETS - AHEAD):
            for j in range(GROUP):
                for c in writes(g - k, lax.rem(g - k, SETS), j):
                    c.wait()
        for k in range(2):
            for c in u_write(g - k, lax.rem(g - k, 2)):
                c.wait()


def attend(first, count, done, perm, pos, base, query, lat_new, rope_new, lat_cache, rope_t, score_scale):
    heads = query.shape[1]
    rank = lat_cache.shape[2]
    seq = lat_cache.shape[1]
    rope_dim = rope_t.shape[1]
    n_groups = count // GROUP
    g0 = first // GROUP
    n_ml = pl.cdiv(count, 128)
    any_spec = pl.BlockSpec(memory_space=pl.ANY)
    return pl.pallas_call(
        functools.partial(attend_kernel, score_scale, n_groups, first, len(done), (128, seq) if first or count == perm.shape[0] else (seq,)),
        grid_spec=pltpu.PrefetchScalarGridSpec(
            num_scalar_prefetch=3,
            grid=(n_groups,),
            in_specs=[
                pl.BlockSpec((GROUP, heads, query.shape[2]), lambda g, *_: (g + g0, 0, 0)),
                pl.BlockSpec((GROUP, rank), lambda g, *_: (g + g0, 0)),
                pl.BlockSpec((GROUP, rope_dim), lambda g, *_: (g + g0, 0)),
            ] + [any_spec] * (2 + len(done)),
            out_specs=[any_spec, any_spec, any_spec,
                       pl.BlockSpec((2, n_ml, heads, 128), lambda g, *_: (0, 0, 0, 0))],
            scratch_shapes=[
                pltpu.VMEM((SETS * GROUP, seq, rank), jnp.bfloat16),
                pltpu.VMEM((SETS * GROUP, rope_dim, seq), jnp.bfloat16),
                pltpu.VMEM((2, rank // 128, heads * GROUP, 128), jnp.float32),
                pltpu.SemaphoreType.DMA((SETS * GROUP,)),
                pltpu.SemaphoreType.DMA((SETS * GROUP,)),
                pltpu.SemaphoreType.DMA((SETS * GROUP,)),
                pltpu.SemaphoreType.DMA((SETS * GROUP,)),
                pltpu.SemaphoreType.DMA((2, rank // 128)),
            ],
        ),
        out_shape=[
            jax.ShapeDtypeStruct(lat_cache.shape, lat_cache.dtype),
            jax.ShapeDtypeStruct(rope_t.shape, rope_t.dtype),
            jax.ShapeDtypeStruct((heads, count, rank), jnp.float32),
            jax.ShapeDtypeStruct((2, n_ml, heads, 128), jnp.float32),
        ],
        input_output_aliases={8: 0, 9: 1} if done else {},
        compiler_params=pltpu.CompilerParams(dimension_semantics=("arbitrary",), vmem_limit_bytes=48 * 1024 * 1024),
        cost_estimate=pl.CostEstimate(flops=16 * count * heads * seq * (2 * rank + rope_dim), bytes_accessed=count * seq * rank * 5,
                                      transcendentals=0),
        name=f"attend{first}_{count}",
    )(perm, pos, base, query, lat_new, rope_new, lat_cache, rope_t, *done)


CH = 4


def row_block(rows):
    return max(d for d in range(8, 65, 8) if rows % d == 0)


def remote(src, dst, ss, rs, dev):
    return pltpu.make_async_remote_copy(src_ref=src, dst_ref=dst, send_sem=ss, recv_sem=rs,
                                        device_id=dev, device_id_type=MESH)


def factors(stats, mine, other, lo, count, f_buf):
    sources = stats.shape[0]
    for b in range(stats.shape[2]):
        m = [stats[s, 0, b, pl.ds(lo, count), :] for s in range(sources)]
        top = functools.reduce(jnp.maximum, m)
        total = sum(jnp.exp(m[s] - top) * stats[s, 1, b, pl.ds(lo, count), :] for s in range(sources))
        total = jnp.maximum(total, 1e-30)
        for slot, s in enumerate((mine, other)):
            f = jnp.exp(stats[s, 0, b, pl.ds(lo, count), :] - top) / total
            f_buf[slot, b * 128:(b + 1) * 128, :] = f.T


def column(f_buf, slot, r0, rb, h):
    f = f_buf[slot, pl.ds(r0, rb), :]
    lane = lax.broadcasted_iota(jnp.int32, f.shape, 1)
    return jnp.sum(jnp.where(lane == h, f, 0.0), axis=1, keepdims=True)


def pair_kernel(u_ref, ml_ref, keep_ref, give_ref, d_buf, own_buf, stats, f_buf,
                d_ss, d_rs, s_ss, s_rs, own_sem, out_sem):
    hh, rows, rank = d_buf.shape
    half = rows // 2
    n_chunk = hh // CH
    dp = lax.axis_index('dp')
    tp = lax.axis_index('tp')
    sp = lax.axis_index('sp')
    n_sp = stats.shape[0]
    core = lax.rem(sp, 2)
    x = sp // 2
    mate = x * 2 + (1 - core)
    peers = [lax.rem(sp + i, n_sp) for i in range(1, n_sp)]
    barrier = pltpu.get_barrier_semaphore()
    for p in peers:
        pl.semaphore_signal(barrier, inc=1, device_id={'dp': dp, 'tp': tp, 'sp': p}, device_id_type=MESH)

    def own_load(k):
        return pltpu.make_async_copy(u_ref.at[pl.ds(core * hh + k * CH, CH)], own_buf.at[lax.rem(k, 2)], own_sem.at[lax.rem(k, 2)])

    for k in range(2):
        own_load(k).start()
    pl.semaphore_wait(barrier, n_sp - 1)

    def stat_send(i):
        return remote(ml_ref, stats.at[sp], s_ss.at[i], s_rs.at[sp], {'dp': dp, 'tp': tp, 'sp': peers[i]})

    def stat_recv(i):
        return remote(ml_ref, stats.at[peers[i]], s_ss.at[i], s_rs.at[peers[i]], {'dp': dp, 'tp': tp, 'sp': peers[i]})

    def d_copy(k):
        return remote(u_ref.at[pl.ds((1 - core) * hh + k * CH, CH)], d_buf.at[pl.ds(k * CH, CH)],
                      d_ss.at[k], d_rs.at[k], {'dp': dp, 'tp': tp, 'sp': mate})

    for i in range(n_sp - 1):
        stat_send(i).start()
    for k in range(n_chunk):
        d_copy(k).start()
    stats[sp] = ml_ref[...]
    for i in range(n_sp - 1):
        stat_recv(i).wait_recv()
    factors(stats, sp, mate, pl.multiple_of(core * hh, 8), hh, f_buf)

    keep = pl.multiple_of(x * half, 8)
    give = pl.multiple_of((1 - x) * half, 8)
    rb = row_block(rows)

    def outs(k):
        hs = pl.ds(k * CH, CH)
        return (pltpu.make_async_copy(d_buf.at[hs, pl.ds(keep, half), :], keep_ref.at[hs], out_sem.at[0, k]),
                pltpu.make_async_copy(d_buf.at[hs, pl.ds(give, half), :], give_ref.at[hs], out_sem.at[1, k]))

    def chunk(k, _):
        own_load(k).wait()
        d_copy(k).wait_recv()
        slot = lax.rem(k, 2)

        def scale(t, _):
            r0 = pl.multiple_of(t * rb, rb)
            for a in range(CH):
                h = k * CH + a
                fo = column(f_buf, 0, r0, rb, h)
                fm = column(f_buf, 1, r0, rb, h)
                d_buf[h, pl.ds(r0, rb), :] = fo * own_buf[slot, a, pl.ds(r0, rb), :] + fm * d_buf[h, pl.ds(r0, rb), :]
            return 0

        lax.fori_loop(0, rows // rb, scale, 0)
        for c in outs(k):
            c.start()

        @pl.when(k + 2 < n_chunk)
        def _():
            own_load(k + 2).start()
        return 0

    lax.fori_loop(0, n_chunk, chunk, 0)
    for i in range(n_sp - 1):
        stat_send(i).wait_send()

    def drain(k, _):
        d_copy(k).wait_send()
        for c in outs(k):
            c.wait()
        return 0

    lax.fori_loop(0, n_chunk, drain, 0)


def pair_reduce(cid, n_sp, u, ml):
    heads, rows, rank = u.shape
    hh = heads // 2
    n_chunk = hh // CH
    dma = pltpu.SemaphoreType.DMA
    any_spec = pl.BlockSpec(memory_space=pl.ANY)
    return pl.pallas_call(
        pair_kernel,
        in_specs=[any_spec, pl.BlockSpec(memory_space=pltpu.VMEM)],
        out_specs=[any_spec, any_spec],
        out_shape=[jax.ShapeDtypeStruct((hh, rows // 2, rank), jnp.float32)] * 2,
        scratch_shapes=[
            pltpu.VMEM((hh, rows, rank), jnp.float32),
            pltpu.VMEM((2, CH, rows, rank), jnp.float32),
            pltpu.VMEM((n_sp,) + ml.shape, jnp.float32),
            pltpu.VMEM((2, ml.shape[1] * 128, hh), jnp.float32),
            dma((n_chunk,)), dma((n_chunk,)), dma((n_sp,)), dma((n_sp,)), dma((2,)), dma((2, n_chunk)),
        ],
        compiler_params=pltpu.CompilerParams(collective_id=cid, has_side_effects=True, vmem_limit_bytes=VMEM_LIMIT),
        cost_estimate=pl.CostEstimate(flops=2_000_000_000, bytes_accessed=20_000_000, transcendentals=0),
        name=f"pair{rows}",
    )(u, ml)


def combine_kernel(n_rest, keep_ref, got_ref, wuv_ref, wout_ref, hid_ref, sel_ref, sel_t_ref, *refs):
    if n_rest:
        u_ref, ml_ref = refs[:2]
        refs = refs[2:]
    (out_ref, att, hid_buf, out_buf, hid_sem, out_sem, keep_buf, got_buf, o_out, o_in, o_all, w_buf, p_buf, y_buf, wuv_buf, k_buf,
     o_ss, o_rs, y_ss, y_rs, h_ss, h_rs, c_ss, c_rs, w_ss, w_rs,
     own_sem, keep_sem, wt_sem, wuv_sem) = refs[:30]
    if n_rest:
        d_buf, own_buf, stats, f_buf, d_ss, d_rs, s_ss, s_rs = refs[30:]
    hh, half, rank = keep_ref.shape
    r_own = half + n_rest
    vdim = wuv_buf.shape[3]
    wh = wuv_buf.shape[2]
    n_chunk = hh // CH
    n_blk, _, bcol = p_buf.shape
    dp = lax.axis_index('dp')
    tp = lax.axis_index('tp')
    sp = lax.axis_index('sp')
    core = lax.rem(sp, 2)
    x = sp // 2
    to_mate = {'dp': dp, 'tp': tp, 'sp': x * 2 + (1 - core)}
    to_x = {'dp': dp, 'tp': tp, 'sp': (1 - x) * 2 + core}
    to_y = {'dp': dp, 'tp': 1 - tp, 'sp': sp}

    barrier = pltpu.get_barrier_semaphore()
    for dev in (to_mate, to_x, to_y):
        pl.semaphore_signal(barrier, inc=1, device_id=dev, device_id_type=MESH)

    def loads(k):
        slot = lax.rem(k, 2)
        hs = pl.ds(k * CH, CH)
        cs = [pltpu.make_async_copy(keep_ref.at[hs], keep_buf.at[slot], keep_sem.at[0, slot]),
              pltpu.make_async_copy(got_ref.at[hs], got_buf.at[slot], keep_sem.at[1, slot])]
        if n_rest:
            cs.append(pltpu.make_async_copy(u_ref.at[pl.ds(core * hh + k * CH, CH)], own_buf.at[slot], own_sem.at[slot]))
        return cs

    def w_load(j):
        col = pl.multiple_of(core * (n_blk * bcol) + j * bcol, 128)
        return pltpu.make_async_copy(wout_ref.at[:, pl.ds(col, bcol)], w_buf.at[lax.rem(j, 2)], wt_sem.at[lax.rem(j, 2)])

    for k in range(2):
        for c in loads(k):
            c.start()

    def wuv_load(a):
        return pltpu.make_async_copy(wuv_ref.at[:, pl.ds(core * hh + a * wh, wh), :], wuv_buf.at[a], wuv_sem.at[a])

    for a in range(hh // wh):
        wuv_load(a).start()
    pl.semaphore_wait(barrier, 3)

    def d_copy(k):
        return remote(u_ref.at[pl.ds((1 - core) * hh + k * CH, CH)], d_buf.at[pl.ds(k * CH, CH)],
                      d_ss.at[k], d_rs.at[k], to_mate)

    if n_rest:
        stat_copy = remote(ml_ref, stats.at[1], s_ss, s_rs, to_mate)
        stat_copy.start()
        for k in range(n_chunk):
            d_copy(k).start()
    for j in range(2):
        w_load(j).start()
    if n_rest:
        stats[0] = ml_ref[...]
        stat_copy.wait_recv()
        factors(stats, 0, 1, pl.multiple_of(core * hh, 8), hh, f_buf)

    def o_copy(k):
        return remote(o_out.at[pl.ds(k * CH, CH)], o_in.at[pl.ds(k * CH, CH)], o_ss.at[k], o_rs.at[k], to_mate)

    rb = row_block(n_rest) if n_rest else 8

    def project_chunk(k, _):
        slot = lax.rem(k, 2)
        for c in loads(k):
            c.wait()
        if n_rest:
            d_copy(k).wait_recv()

        @pl.when(lax.rem(k, wh // CH) == 0)
        def _():
            wuv_load(k // (wh // CH)).wait()
            k_buf[...] = wuv_buf[k // (wh // CH)].astype(jnp.float32).reshape(k_buf.shape)

        for a in range(CH):
            h = k * CH + a
            wuv_h = k_buf[pl.ds(lax.rem(h, wh), rank, stride=wh), :].astype(jnp.bfloat16)
            u = keep_buf[slot, a] + got_buf[slot, a]
            if n_rest:
                parts = [u]
                for r0 in range(0, n_rest, rb):
                    fo = column(f_buf, 0, r0, rb, h)
                    fm = column(f_buf, 1, r0, rb, h)
                    parts.append(fo * own_buf[slot, a, pl.ds(r0, rb), :] + fm * d_buf[h, pl.ds(r0, rb), :])
                u = jnp.concatenate(parts, axis=0)
            o = jnp.dot(u.astype(jnp.bfloat16), wuv_h, preferred_element_type=jnp.float32).astype(jnp.bfloat16)
            o_all[:, pl.ds(pl.multiple_of((core * hh + h) * vdim, 128), vdim)] = o
            o_out[h] = o.astype(jnp.float32)

        o_copy(k).start()

        @pl.when(k + 2 < n_chunk)
        def _():
            for c in loads(k + 2):
                c.start()
        return 0

    lax.fori_loop(0, n_chunk, project_chunk, 0)

    def place_chunk(k, _):
        o_copy(k).wait_recv()

        for a in range(CH):
            h = k * CH + a
            o_all[:, pl.ds(pl.multiple_of(((1 - core) * hh + h) * vdim, 128), vdim)] = o_in[h].astype(jnp.bfloat16)
        return 0

    lax.fori_loop(0, n_chunk, place_chunk, 0)

    mine = core * n_blk
    theirs = (1 - core) * n_blk

    def y_copy(j):
        return remote(p_buf.at[j], y_buf.at[j], y_ss.at[j], y_rs.at[j], to_y)

    def c_copy(j):
        return remote(att.at[x, mine + j], att.at[x, mine + j], c_ss.at[j], c_rs.at[j], to_mate)

    def h_copy(j):
        return remote(att.at[x, mine + j], att.at[x, mine + j], h_ss.at[j], h_rs.at[j], to_x)

    def w_copy(j):
        return remote(att.at[1 - x, mine + j], att.at[1 - x, mine + j], w_ss.at[j], w_rs.at[j], to_mate)

    def hid_load(kind, j):
        col = pl.multiple_of(((theirs if kind else mine) + j) * bcol, 128)
        slot = 2 * kind + lax.rem(j, 2)
        return pltpu.make_async_copy(hid_ref.at[:, pl.ds(col, bcol)], hid_buf.at[slot], hid_sem.at[slot])

    def out_store(kind, j):
        col = pl.multiple_of(((theirs if kind else mine) + j) * bcol, 128)
        slot = 2 * kind + lax.rem(j, 2)
        return pltpu.make_async_copy(out_buf.at[slot], out_ref.at[:, pl.ds(col, bcol)], out_sem.at[slot])

    def total(j):
        y_copy(j).wait_recv()
        att[x, mine + j] = y_buf[j] + p_buf[j]
        h_copy(j).start()
        c_copy(j).start()

    def forward(j):
        h_copy(j).wait_recv()
        w_copy(j).start()

    def finalize(kind, j):
        slot = 2 * kind + lax.rem(j, 2)
        blk = (theirs if kind else mine) + j
        hid_load(kind, j).wait()
        hid = jnp.dot(sel_ref[...], hid_buf[slot], preferred_element_type=jnp.float32)
        parts = [att[0, blk, :half], att[1, blk, :half]]
        if n_rest:
            parts.append(att[0, blk, half:])
        rows_s = (hid + jnp.concatenate(parts, axis=0)).astype(jnp.bfloat16)

        @pl.when(j >= 2)
        def _():
            out_store(kind, j - 2).wait()

        out_buf[slot] = jnp.dot(sel_t_ref[...], rows_s, preferred_element_type=jnp.float32).astype(out_buf.dtype)
        out_store(kind, j).start()

        @pl.when(j + 2 < n_blk)
        def _():
            hid_load(kind, j + 2).start()

    def finalize_mate(j):
        pltpu.make_async_remote_copy(src_ref=att.at[x, theirs + j], dst_ref=att.at[x, theirs + j], send_sem=c_ss.at[j],
                                     recv_sem=c_rs.at[j], device_id=to_mate, device_id_type=MESH).wait_recv()
        pltpu.make_async_remote_copy(src_ref=att.at[1 - x, theirs + j], dst_ref=att.at[1 - x, theirs + j], send_sem=w_ss.at[j],
                                     recv_sem=w_rs.at[j], device_id=to_mate, device_id_type=MESH).wait_recv()
        finalize(1, j)

    for kind in range(2):
        for j in range(2):
            hid_load(kind, j).start()
    early = (4, 8, 11)
    lag = len(early)

    def block(j, _):
        w_load(j).wait()
        p_buf[j] = jnp.dot(o_all[...], w_buf[lax.rem(j, 2)], preferred_element_type=jnp.float32)
        y_copy(j).start()

        @pl.when(j + 2 < n_blk)
        def _():
            w_load(j + 2).start()

        for i, at in enumerate(early):
            @pl.when(j == at)
            def _(i=i):
                total(i)
        return 0

    lax.fori_loop(0, n_blk, block, 0)

    def finish(j, _):
        @pl.when(j < n_blk)
        def _():
            total(j)

        @pl.when(j - lag < n_blk)
        def _():
            forward(j - lag)
            finalize(0, j - lag)

        @pl.when(j - lag >= 1)
        def _():
            finalize_mate(j - lag - 1)
        return 0

    lax.fori_loop(lag, n_blk + lag + 1, finish, 0)

    def drain(k, _):
        if n_rest:
            d_copy(k).wait_send()
        o_copy(k).wait_send()
        return 0

    lax.fori_loop(0, n_chunk, drain, 0)
    if n_rest:
        stat_copy.wait_send()

    def drain_blocks(j, _):
        y_copy(j).wait_send()
        h_copy(j).wait_send()
        c_copy(j).wait_send()
        w_copy(j).wait_send()
        return 0

    lax.fori_loop(0, n_blk, drain_blocks, 0)
    for kind in range(2):
        for j in range(n_blk - 2, n_blk):
            out_store(kind, j).wait()


def combine(cid, keep, got, wuv, wout, hidden, sel, sel_t, rest):
    hh, half, rank = keep.shape
    n_rest = rest[0].shape[1] if rest else 0
    vdim = wuv.shape[2]
    depth, width = wout.shape
    r_own = half + n_rest
    bcol = 256
    n_blk = width // 2 // bcol
    n_chunk = hh // CH
    dma = pltpu.SemaphoreType.DMA
    any_spec = pl.BlockSpec(memory_space=pl.ANY)
    vmem_spec = pl.BlockSpec(memory_space=pltpu.VMEM)
    rows = hidden.shape[0]
    scratch = [
        pltpu.VMEM((2, 2 * n_blk, r_own, bcol), jnp.float32),
        pltpu.VMEM((4, rows, bcol), jnp.bfloat16),
        pltpu.VMEM((4, rows, bcol), jnp.bfloat16),
        dma((4,)), dma((4,)),
        pltpu.VMEM((2, CH, half, rank), jnp.float32),
        pltpu.VMEM((2, CH, half, rank), jnp.float32),
        pltpu.VMEM((hh, r_own, vdim), jnp.float32),
        pltpu.VMEM((hh, r_own, vdim), jnp.float32),
        pltpu.VMEM((r_own, depth), jnp.bfloat16),
        pltpu.VMEM((2, depth, bcol), jnp.bfloat16),
        pltpu.VMEM((n_blk, r_own, bcol), jnp.float32),
        pltpu.VMEM((n_blk, r_own, bcol), jnp.float32),
        pltpu.VMEM((hh // 8, rank, 8, vdim), jnp.bfloat16),
        pltpu.VMEM((rank * 8, vdim), jnp.float32),
    ] + [dma((n_chunk,))] * 2 + [dma((n_blk,))] * 8 + [dma((2,)), dma((2, 2)), dma((2,)), dma((hh // 8,))]
    if rest:
        scratch += [
            pltpu.VMEM((hh, n_rest, rank), jnp.float32),
            pltpu.VMEM((2, CH, n_rest, rank), jnp.float32),
            pltpu.VMEM((2,) + rest[1].shape, jnp.float32),
            pltpu.VMEM((2, rest[1].shape[1] * 128, hh), jnp.float32),
            dma((n_chunk,)), dma((n_chunk,)), dma(()), dma(()),
        ]
    return pl.pallas_call(
        functools.partial(combine_kernel, n_rest),
        in_specs=[any_spec] * 5 + [vmem_spec, vmem_spec] + ([any_spec, vmem_spec] if rest else []),
        out_specs=any_spec,
        out_shape=jax.ShapeDtypeStruct(hidden.shape, hidden.dtype),
        scratch_shapes=scratch,
        compiler_params=pltpu.CompilerParams(collective_id=cid, has_side_effects=True, vmem_limit_bytes=VMEM_LIMIT),
        name=f"combine{2 * half}",
    )(keep, got, wuv, wout, hidden, sel, sel_t, *rest)


def solution(mesh):
    row_spec = P('dp', None)
    cache_spec = P('dp', 'sp', None)
    head_spec = P(None, 'tp', None)
    in_specs = (row_spec, cache_spec, cache_spec, P('dp'), P(), P(), P(), P(), head_spec, head_spec, head_spec, P('tp', None))
    out_specs = (row_spec, cache_spec, cache_spec)
    n_sp = mesh.shape['sp']

    def local_step(hidden, lat_cache, rope_cache, positions, w_dq, gain_q, w_dkv, gain_kv, w_uq, w_uk, w_uv, w_out):
        rows = hidden.shape[0]
        seq = lat_cache.shape[1]
        heads = w_uk.shape[1]
        score_scale = YARN_MSCALE ** 2 / math.sqrt(w_uq.shape[2])
        sp = lax.axis_index('sp')

        idx = jnp.arange(rows)
        before = (positions[None, :] > positions[:, None]) | ((positions[None, :] == positions[:, None]) & (idx[None, :] < idx[:, None]))
        rank = jnp.sum(before.astype(jnp.int32), axis=1)
        sel = rank[None, :] == idx[:, None]
        perm = jnp.sum(jnp.where(sel, idx[None, :], 0), axis=1).astype(jnp.int32)
        pos_s = jnp.sum(jnp.where(sel, positions[None, :], 0), axis=1).astype(jnp.int32)
        sel16 = sel.astype(jnp.bfloat16)
        hidden_s = jnp.dot(sel16, hidden, preferred_element_type=jnp.float32).astype(jnp.bfloat16)

        query, lat_new, rope_new = project_inputs(hidden_s, pos_s, w_dq, gain_q, w_dkv, gain_kv, w_uq, w_uk)
        base = (sp * seq).astype(jnp.int32).reshape(1)
        rope_t = rope_cache.transpose(0, 2, 1)
        n_over = jnp.sum((positions >= (n_sp // 2) * seq).astype(jnp.int32))
        sizes = sorted({min(rows, max(16, s * rows // 256)) for s in SIZES})
        which = sum((n_over > s).astype(jnp.int32) for s in sizes[:-1])
        swap = [(i, (i + n_sp // 2) % n_sp) for i in range(n_sp)]

        def branch(n_cross, cid):
            def run(perm, pos_s, base, query, lat_new, rope_new, lat_cache, rope_t, w_uv, w_out, hidden, sel16):
                common = (perm, pos_s, base, query, lat_new, rope_new, lat_cache, rope_t, score_scale)
                lat_out, rope_out, u_first, ml_first = attend(0, n_cross, (), *common)
                keep, give = pair_reduce(2 * cid, n_sp, u_first, ml_first)
                got = lax.ppermute(give, 'sp', swap)
                rest = ()
                if n_cross < rows:
                    lat_out, rope_out, *rest = attend(n_cross, rows - n_cross, (lat_out, rope_out), *common)
                out = combine(2 * cid + 1, keep, got, w_uv, w_out, hidden, sel16, sel16.T, rest)
                return out, lat_out, rope_out
            return run

        out, lat_out, rope_out = lax.switch(which, [branch(s, i) for i, s in enumerate(sizes)], perm, pos_s, base, query,
                                            lat_new, rope_new, lat_cache, rope_t, w_uv, w_out, hidden, sel16)
        return out, lat_out, rope_out.transpose(0, 2, 1)

    return jax.shard_map(local_step, mesh=mesh, in_specs=in_specs, out_specs=out_specs, check_vma=False)
```
